256 devices in a mesh: tp: 64 (over y, x, z_hi), col: 4 (over z_lo, core).
Axes of the slice: x: 4, y: 4, z: 8 (z_hi: 4, z_lo: 2; z = z_hi * 2 + z_lo), core: 2. Of those that a mesh axis runs over, the one named last changes fastest.
Arguments:
- gate_in: bfloat16 [1024, 53248], P('col', 'tp'), may hold values from -6 to 6
- up_in: bfloat16 [1024, 53248], P('col', 'tp'), may hold values from -6 to 6
- down_weight: bfloat16 [53248, 16384], P('tp', 'col'), may hold values from -0.02734375 to 0.02734375
- residual: bfloat16 [1024, 16384], P('tp', 'col'), may hold values from -30 to 30
- norm_gain: bfloat16 [16384], P('col'), may hold values from 0.5 to 1.5
Outputs:
- stream: bfloat16 [1024, 16384], P('tp', 'col')
- normed: bfloat16 [1024, 16384], P('tp', 'col')
The draws below stay inside these ranges and needn't reach their ends.
All inputs are finite; a program needn't handle non-finite values.
Results may differ from the reference program's by a relative error of at most 0.0034.
Values may be sent and summed in bfloat16 or wider, within the bound.
A program may use at most 128 MiB of HBM per device.

```python
import math
import jax
import jax.numpy as jnp
from jax import lax

D = 16384
FF = 53248
TOKENS = 1024


def draw_residual(key, part):
    key_rows = jax.random.fold_in(key, 11)
    key_values = jax.random.fold_in(key, 23)
    row_scale = jnp.exp(jax.random.uniform(key_rows, (TOKENS, 1), jnp.float32, math.log(0.3), math.log(3.0)))
    ramp = jnp.arange(D, dtype=jnp.float32) / (D - 1)
    col_scale = 0.5 * jnp.exp(ramp * math.log(3.0))
    values = jnp.clip(jax.random.normal(key_values, (TOKENS, D), jnp.float32), -4.0, 4.0)
    return (row_scale * col_scale[None, :] * values).astype(jnp.bfloat16)


def levels(stream_key, extent, shards, smallest, high):
    def one(position, parts):
        draws = jax.random.uniform(jax.random.fold_in(jax.random.fold_in(stream_key, 6), position), (parts,), jnp.float32, smallest / len(shards), high / len(shards))
        return jnp.repeat(jnp.exp(draws), extent[position] // parts).reshape((-1,) + (1,) * (len(extent) - position - 1))

    factor_of = one(*shards[0])
    for cut in shards[1:]:
        factor_of = factor_of * one(*cut)
    return factor_of


def noise(key, dims, scale, most, cuts=(), kind=jnp.bfloat16):
    drawn = scale * jax.random.normal(key, dims, jnp.float32)
    if cuts:
        drawn = drawn * levels(key, dims, cuts, -0.22, 0.18)
    return jnp.clip(drawn, -most, most).astype(kind)


def setup_inputs(seed: int = 0) -> dict:
    arg_keys = jax.random.split(jax.random.key(seed), 6)
    return {
        "gate_in": noise(arg_keys[0], (TOKENS, FF), 1.0, 6.0, ((0, 4), (1, 64))),
        "up_in": noise(arg_keys[1], (TOKENS, FF), 1.0, 6.0, ((0, 4), (1, 64))),
        "down_weight": noise(arg_keys[2], (FF, D), FF ** -0.5, 0.02734375, ((0, 64), (1, 4))),
        "residual": draw_residual(jax.random.fold_in(arg_keys[5], 71), 0),
        "norm_gain": jnp.clip(1.0 + 0.1 * jax.random.normal(arg_keys[4], (D,), jnp.float32), 0.5, 1.5).astype(jnp.bfloat16),
    }


def reference(gate_in, up_in, down_weight, residual, norm_gain):
    hidden = (jax.nn.silu(gate_in.astype(jnp.float32)) * up_in.astype(jnp.float32)).astype(jnp.bfloat16)
    branch = jnp.dot(hidden, down_weight, preferred_element_type=jnp.float32)
    summed = residual.astype(jnp.float32) + branch
    mean_square = lax.optimization_barrier(jnp.mean(summed * summed, axis=1, keepdims=True))
    scaled = summed * lax.rsqrt(mean_square + 1e-05) * norm_gain.astype(jnp.float32)[None, :]
    return (summed.astype(jnp.bfloat16), scaled.astype(jnp.bfloat16))
```

```python
import functools

import jax
import jax.numpy as jnp
from jax import lax
from jax.experimental import pallas as pl
from jax.experimental.pallas import tpu as pltpu
from jax.sharding import Mesh
from jax.sharding import PartitionSpec as P

F32 = jnp.float32
BF16 = jnp.bfloat16
D = 16384
N = 4096
K = 832
KP = 896
TILE = 512
WIDTHS = (2048, 2048)
STARTS = (0, 2048)
COLOURS = ("x", "y")
LAST = F32


def kernel(
    gate_hbm, up_hbm, w_hbm, res_ref, gain_ref, stream_ref, normed_ref,
    gate_v, up_v, w_v, h,
    p32_x, p16_x, p32_y, p16_y,
    ra_x, rb_x, rc_x, c_x, ra_y, rb_y, rc_y, c_y,
    q32_x, q16_x, q32_y, q16_y,
    r2_x, c2_x, r2_y, c2_y,
    t32_x, t16_x, t32_y, t16_y,
    r3_x, c3_x, r3_y, c3_y,
    sq_own, sq_in,
    in_sem, w_sem, ag_send, ag_recv, s1_send, s1_recv, s2_send, s2_recv, s3_send, s3_recv, n_send, n_recv,
):
    x, y, hi, lo, core = (lax.axis_index(a) for a in ("x", "y", "h", "l", "c"))

    def ring(axis, index, step):
        return {axis: lax.rem(index + step, 4)}

    sibling = {"c": 1 - core}
    across = {"l": 1 - lo}
    diagonal = {"l": 1 - lo, "c": 1 - core}
    partners = [sibling, across, diagonal]
    for axis, index in (("x", x), ("y", y), ("h", hi)):
        partners += [ring(axis, index, 1), ring(axis, index, 3)]

    barrier = pltpu.get_barrier_semaphore()
    for who in partners:
        pl.semaphore_signal(barrier, inc=1, device_id=who, device_id_type=pl.DeviceIdType.MESH)

    get_gate = pltpu.make_async_copy(gate_hbm, gate_v, in_sem.at[0])
    get_up = pltpu.make_async_copy(up_hbm, up_v, in_sem.at[1])
    get_gate.start()
    get_up.start()

    def get_w(j):
        cols = pl.ds(pl.multiple_of(j * TILE, TILE), TILE)
        return pltpu.make_async_copy(w_hbm.at[:, cols], w_v.at[pl.ds(0, K), cols], w_sem.at[j])

    for j in range(N // TILE):
        get_w(j).start()
    w_v[K:, :] = jnp.zeros((KP - K, N), BF16)
    get_gate.wait()
    get_up.wait()

    for k in range(KP // 128):
        depth = min(128, K - k * 128)
        g = gate_v[k * 128 : k * 128 + depth, :].astype(F32)
        u = up_v[k * 128 : k * 128 + depth, :].astype(F32)
        act = g / (1.0 + jnp.exp(-g)) * u
        if depth < 128:
            act = jnp.concatenate([act, jnp.zeros((128 - depth, 256), F32)], axis=0)
        h[0, :, k * 128 : (k + 1) * 128] = act.T.astype(BF16)

    pl.semaphore_wait(barrier, len(partners))

    def remote(src, dst, send, recv, who):
        return pltpu.make_async_remote_copy(
            src_ref=src, dst_ref=dst, send_sem=send, recv_sem=recv,
            device_id=who, device_id_type=pl.DeviceIdType.MESH,
        )

    gathers = [
        remote(h.at[0], h.at[1], ag_send.at[0], ag_recv.at[0], sibling),
        remote(h.at[0], h.at[2], ag_send.at[1], ag_recv.at[1], across),
        remote(h.at[2], h.at[3], ag_send.at[2], ag_recv.at[2], sibling),
    ]
    gathers[1].start()
    gathers[0].start()

    blocks = (2 * lo + core, 2 * lo + 1 - core, 2 * (1 - lo) + core, 2 * (1 - lo) + 1 - core)
    roles = [lax.rem(b + 4 - y, 4) for b in blocks]

    def rows(index, step, size):
        return pl.ds(pl.multiple_of(lax.rem(index + step, 4) * size, size), size)

    wx, wy = WIDTHS
    hx, hy = wx // 2, wy // 2

    def product(i, start, width, p32, p16, slot, first):
        def step(j, carry):
            if first:
                get_w(start // TILE + j).wait()
            cols = pl.ds(pl.multiple_of(j * TILE, TILE), TILE)
            from_cols = pl.ds(pl.multiple_of(start + j * TILE, TILE), TILE)
            part = jnp.dot(h[i], w_v[:, from_cols], preferred_element_type=F32)
            p32[slot, :, cols] = part
            p16[slot, :, cols] = part.astype(BF16)
            return carry

        lax.fori_loop(0, width // TILE, step, 0)

    def first_x(kind, i):
        sems = s1_send.at[0, kind, i], s1_recv.at[0, kind, i]
        low, high = pl.ds(0, hx), pl.ds(hx, hx)
        ahead, behind = ring("x", x, 1), ring("x", x, 3)
        return (
            lambda: remote(p16_x.at[i, rows(x, 2, 64), low], ra_x.at[0, i], *sems, ahead),
            lambda: remote(p16_x.at[i, rows(x, 2, 64), high], ra_x.at[1, i], *sems, behind),
            lambda: remote(p16_x.at[i, rows(x, 1, 64), high], rb_x.at[0, i], *sems, ahead),
            lambda: remote(p16_x.at[i, rows(x, 3, 64), low], rb_x.at[1, i], *sems, behind),
            lambda: remote(c_x.at[0, i], rc_x.at[0, i], *sems, ahead),
            lambda: remote(c_x.at[1, i], rc_x.at[1, i], *sems, behind),
        )[kind]()

    def first_y(kind, q):
        sems = s1_send.at[1, kind, q], s1_recv.at[1, kind, q]
        low, high = pl.ds(0, hy), pl.ds(hy, hy)
        ahead, behind = ring("y", y, 1), ring("y", y, 3)
        return (
            lambda: remote(p16_y.at[2, rows(x, q, 64), low], ra_y.at[0, q], *sems, ahead),
            lambda: remote(p16_y.at[2, rows(x, q, 64), high], ra_y.at[1, q], *sems, behind),
            lambda: remote(p16_y.at[1, rows(x, q, 64), high], rb_y.at[0, q], *sems, ahead),
            lambda: remote(p16_y.at[3, rows(x, q, 64), low], rb_y.at[1, q], *sems, behind),
            lambda: remote(c_y.at[0, q], rc_y.at[0, q], *sems, ahead),
            lambda: remote(c_y.at[1, q], rc_y.at[1, q], *sems, behind),
        )[kind]()

    order = (2, 1, 3, 0)

    def x_product(i, first=False):
        product(i, STARTS[0], wx, p32_x, p16_x, i, first)
        for kind in (0, 1, 2, 3):
            first_x(kind, i).start()

    def y_product(i, first=False):
        role = roles[i]
        product(i, STARTS[1], wy, p32_y, p16_y, role, first)
        for r, kinds in ((2, (0, 1)), (1, (2,)), (3, (3,))):

            @pl.when(role == r)
            def _():
                for q in order:
                    for kind in kinds:
                        first_y(kind, q).start()

    def x_relay(i):
        for s, step in ((0, 1), (1, 3)):
            first_x(s, i).wait_recv()
            mine = p32_x[i, rows(x, step, 64), s * hx : (s + 1) * hx]
            c_x[s, i] = (mine + ra_x[s, i].astype(F32)).astype(BF16)
            first_x(4 + s, i).start()

    def y_relay(s, q):
        first_y(s, q).wait_recv()
        mine = p32_y[1 + 2 * s, rows(x, q, 64), s * hy : (s + 1) * hy]
        c_y[s, q] = (mine + ra_y[s, q].astype(F32)).astype(BF16)
        first_y(4 + s, q).start()

    def y_relays(i):
        for s, r in ((0, 1), (1, 3)):

            @pl.when(roles[i] == r)
            def _():
                for q in order:
                    y_relay(s, q)

    def second(colour, kind):
        sems = s2_send.at[colour, kind], s2_recv.at[colour, kind]
        q16, r2, c2 = ((q16_x, r2_x, c2_x), (q16_y, r2_y, c2_y))[colour]
        half = (hx, hy)[colour]
        low, high = pl.ds(0, half), pl.ds(half, half)
        axis, index = (("y", y), ("x", x))[colour]
        ahead, behind = ring(axis, index, 1), ring(axis, index, 3)
        return (
            lambda: remote(q16.at[2, :, low], r2.at[0], *sems, ahead),
            lambda: remote(q16.at[2, :, high], r2.at[1], *sems, behind),
            lambda: remote(q16.at[1, :, high], r2.at[2], *sems, ahead),
            lambda: remote(q16.at[3, :, low], r2.at[3], *sems, behind),
            lambda: remote(c2.at[0], r2.at[4], *sems, ahead),
            lambda: remote(c2.at[1], r2.at[5], *sems, behind),
        )[kind]()

    def x_finish(i):
        for kind in (2, 3, 4, 5):
            first_x(kind, i).wait_recv()
        role = roles[i]
        low = p32_x[i, rows(x, 0, 64), :hx] + rc_x[0, i].astype(F32) + rb_x[1, i].astype(F32)
        q32_x[role, :, :hx] = low
        q16_x[role, :, :hx] = low.astype(BF16)
        high = p32_x[i, rows(x, 0, 64), hx:] + rb_x[0, i].astype(F32) + rc_x[1, i].astype(F32)
        q32_x[role, :, hx:] = high
        q16_x[role, :, hx:] = high.astype(BF16)
        for r, kinds in ((2, (0, 1)), (1, (2,)), (3, (3,))):

            @pl.when(role == r)
            def _():
                for kind in kinds:
                    second(0, kind).start()

    def y_finish(q):
        for kind in (2, 3, 4, 5):
            first_y(kind, q).wait_recv()
        low = p32_y[0, rows(x, q, 64), :hy] + rc_y[0, q].astype(F32) + rb_y[1, q].astype(F32)
        q32_y[q, :, :hy] = low
        q16_y[q, :, :hy] = low.astype(BF16)
        high = p32_y[0, rows(x, q, 64), hy:] + rb_y[0, q].astype(F32) + rc_y[1, q].astype(F32)
        q32_y[q, :, hy:] = high
        q16_y[q, :, hy:] = high.astype(BF16)
        for kind in {2: (0, 1), 1: (2,), 3: (3,), 0: ()}[q]:
            second(1, kind).start()

    def second_relay(colour, s):
        q32, r2, c2 = ((q32_x, r2_x, c2_x), (q32_y, r2_y, c2_y))[colour]
        half = (hx, hy)[colour]
        second(colour, s).wait_recv()
        mine = q32[1 + 2 * s, :, s * half : (s + 1) * half]
        c2[s] = (mine + r2[s].astype(F32)).astype(BF16)
        second(colour, 4 + s).start()

    def third(colour, kind):
        sems = s3_send.at[colour, kind], s3_recv.at[colour, kind]
        t16, r3, c3 = ((t16_x, r3_x, c3_x), (t16_y, r3_y, c3_y))[colour]
        half = (hx, hy)[colour]
        low, high = pl.ds(0, half), pl.ds(half, half)
        ahead, behind = ring("h", hi, 1), ring("h", hi, 3)
        return (
            lambda: remote(t16.at[rows(hi, 2, 16), low], r3.at[0], *sems, ahead),
            lambda: remote(t16.at[rows(hi, 2, 16), high], r3.at[1], *sems, behind),
            lambda: remote(t16.at[rows(hi, 1, 16), high], r3.at[2], *sems, ahead),
            lambda: remote(t16.at[rows(hi, 3, 16), low], r3.at[3], *sems, behind),
            lambda: remote(c3.at[0], r3.at[4], *sems, ahead),
            lambda: remote(c3.at[1], r3.at[5], *sems, behind),
        )[kind]()

    def second_finish(colour):
        q32, r2, t32, t16 = ((q32_x, r2_x, t32_x, t16_x), (q32_y, r2_y, t32_y, t16_y))[colour]
        half = (hx, hy)[colour]
        for kind in (2, 3, 4, 5):
            second(colour, kind).wait_recv()
        low = q32[0, :, :half] + r2[4].astype(F32) + r2[3].astype(F32)
        t32[:, :half] = low
        t16[:, :half] = low.astype(LAST)
        high = q32[0, :, half:] + r2[2].astype(F32) + r2[5].astype(F32)
        t32[:, half:] = high
        t16[:, half:] = high.astype(LAST)
        for kind in (0, 1, 2, 3):
            third(colour, kind).start()

    def third_relay(colour, s):
        t32, r3, c3 = ((t32_x, r3_x, c3_x), (t32_y, r3_y, c3_y))[colour]
        half = (hx, hy)[colour]
        third(colour, s).wait_recv()
        mine = t32[rows(hi, 1 + 2 * s, 16), s * half : (s + 1) * half]
        c3[s] = (mine + r3[s].astype(F32)).astype(LAST)
        third(colour, 4 + s).start()

    def third_finish(colour):
        t32, r3 = ((t32_x, r3_x), (t32_y, r3_y))[colour]
        half, start = (hx, hy)[colour], STARTS[colour]
        for kind in (2, 3, 4, 5):
            third(colour, kind).wait_recv()
        squares = jnp.zeros((16, 128), F32)
        for s, (a, b) in ((0, (4, 3)), (1, (2, 5))):
            for j in range(half // 128):
                here = s * half + j * 128
                cols = pl.ds(j * 128, 128)
                summed = t32[rows(hi, 0, 16), pl.ds(here, 128)] + r3[a, :, cols].astype(F32) + r3[b, :, cols].astype(F32)
                summed = summed + res_ref[:, pl.ds(start + here, 128)].astype(F32)
                t32[rows(hi, 0, 16), pl.ds(here, 128)] = summed
                stream_ref[:, pl.ds(start + here, 128)] = summed.astype(BF16)
                squares = squares + summed * summed
        return squares

    x_product(0, first=True)
    gathers[0].wait_recv()
    x_product(1)
    y_product(0, first=True)
    y_product(1)
    x_relay(0)
    gathers[1].wait_recv()
    gathers[2].start()
    x_product(2)
    y_product(2)
    gathers[2].wait_recv()
    x_product(3)
    y_product(3)
    x_relay(1)
    y_relays(0)
    y_relays(1)
    x_relay(2)
    y_relays(2)
    x_finish(0)
    x_relay(3)
    y_relays(3)
    x_finish(1)
    x_finish(2)
    x_finish(3)
    second_relay(0, 0)
    second_relay(0, 1)
    for q in order:
        y_finish(q)
    second_finish(0)
    second_relay(1, 0)
    second_relay(1, 1)
    third_relay(0, 0)
    third_relay(0, 1)
    second_finish(1)
    total = third_finish(0)
    third_relay(1, 0)
    third_relay(1, 1)
    total = total + third_finish(1)

    sq_own[...] = total
    exchange = [
        remote(sq_own, sq_in.at[i], n_send.at[i], n_recv.at[i], who)
        for i, who in enumerate((sibling, across, diagonal))
    ]
    for copy in exchange:
        copy.start()
    for copy in exchange:
        copy.wait_recv()
    for i in range(3):
        total = total + sq_in[i]
    scale = lax.rsqrt(jnp.sum(total, axis=1, keepdims=True) / D + 1e-05)
    for colour, t32 in enumerate((t32_x, t32_y)):
        for j in range(WIDTHS[colour] // 128):
            at = STARTS[colour] + j * 128
            gain = gain_ref[at // 128 : at // 128 + 1, :].astype(F32)
            scaled = t32[rows(hi, 0, 16), pl.ds(j * 128, 128)] * scale * gain
            normed_ref[:, pl.ds(at, 128)] = scaled.astype(BF16)

    for copy in gathers + exchange:
        copy.wait_send()
    for kind in range(6):
        for piece in range(4):
            first_x(kind, piece).wait_send()
            first_y(kind, piece).wait_send()
        for colour in range(2):
            second(colour, kind).wait_send()
            third(colour, kind).wait_send()


def body(gate_in, up_in, down_weight, residual, norm_gain):
    dma = pltpu.SemaphoreType.DMA
    scratch = [
        pltpu.VMEM((K, 256), BF16),
        pltpu.VMEM((K, 256), BF16),
        pltpu.VMEM((KP, N), BF16),
        pltpu.VMEM((4, 256, KP), BF16),
    ]
    for width in WIDTHS:
        scratch += [pltpu.VMEM((4, 256, width), F32), pltpu.VMEM((4, 256, width), BF16)]
    for width in WIDTHS:
        scratch += [pltpu.VMEM((2, 4, 64, width // 2), BF16)] * 4
    for width in WIDTHS:
        scratch += [pltpu.VMEM((4, 64, width), F32), pltpu.VMEM((4, 64, width), BF16)]
    for width in WIDTHS:
        scratch += [pltpu.VMEM((6, 64, width // 2), BF16), pltpu.VMEM((2, 64, width // 2), BF16)]
    for width in WIDTHS:
        scratch += [pltpu.VMEM((64, width), F32), pltpu.VMEM((64, width), LAST)]
    for width in WIDTHS:
        scratch += [pltpu.VMEM((6, 16, width // 2), LAST), pltpu.VMEM((2, 16, width // 2), LAST)]
    scratch += [
        pltpu.VMEM((16, 128), F32),
        pltpu.VMEM((3, 16, 128), F32),
        dma((2,)),
        dma((N // TILE,)),
        dma((3,)),
        dma((3,)),
        dma((2, 6, 4)),
        dma((2, 6, 4)),
        dma((2, 6)),
        dma((2, 6)),
        dma((2, 6)),
        dma((2, 6)),
        dma((3,)),
        dma((3,)),
    ]
    anywhere = pl.BlockSpec(memory_space=pl.ANY)
    vmem = pl.BlockSpec(memory_space=pltpu.VMEM)
    out = jax.ShapeDtypeStruct((16, N), BF16)
    return pl.pallas_call(
        kernel,
        out_shape=(out, out),
        in_specs=[anywhere, anywhere, anywhere, vmem, vmem],
        out_specs=(vmem, vmem),
        scratch_shapes=scratch,
        compiler_params=pltpu.CompilerParams(
            collective_id=0, has_side_effects=True, vmem_limit_bytes=60 * 1024 * 1024
        ),
    )(gate_in.T, up_in.T, down_weight, residual, norm_gain.reshape(N // 128, 128))


def solution(mesh):
    split = Mesh(mesh.devices.reshape(4, 4, 4, 2, 2), ("y", "x", "h", "l", "c"))
    tp, col = ("y", "x", "h"), ("l", "c")
    return jax.shard_map(
        body,
        mesh=split,
        in_specs=(P(col, tp), P(col, tp), P(tp, col), P(tp, col), P(col)),
        out_specs=(P(tp, col), P(tp, col)),
        check_vma=False,
    )
```

```python
import functools

import jax
import jax.numpy as jnp
from jax import lax
from jax.experimental import pallas as pl
from jax.experimental.pallas import tpu as pltpu
from jax.sharding import Mesh
from jax.sharding import PartitionSpec as P

F32 = jnp.float32
BF16 = jnp.bfloat16
D = 16384
N = 4096
K = 832
KP = 896
TILE = 512
VMEM_LIMIT = 58 * 1024 * 1024
WX = 2048
WY = N - WX
HX, QY = WX // 2, WY // 4
HY = QY // 2
LAST_X = BF16
LAST_Y = F32


def kernel(
    gate_hbm, up_hbm, w_hbm, res_ref, gain_ref, out_ref,
    gate_v, up_v, w_v, h,
    p32_x, p16_x, p32_y, p16_y,
    ra_x, rb_x, rc_x, c_x, ra_y, rb_y, rc_y, c_y,
    r2_x, c2_x, r2_y, c2_y,
    t32_x, t16_x, t32_y, t16_y,
    r3_x, c3_x, r3_y, c3_y,
    u_y, turned, summed, sq_own, sq_in,
    in_sem, w_sem, ag_send, ag_recv, s1_send, s1_recv, sx2_send, sx2_recv, sy2_send, sy2_recv,
    sx3_send, sx3_recv, sy3_send, sy3_recv, turn_send, turn_recv, n_send, n_recv,
):
    x, y, hi, lo, core = (lax.axis_index(a) for a in ("x", "y", "h", "l", "c"))
    scope = jax.named_scope

    def ring(axis, index, step):
        return {axis: lax.rem(index + step, 4)}

    get_gate = pltpu.make_async_copy(gate_hbm, gate_v, in_sem.at[0])
    get_up = pltpu.make_async_copy(up_hbm, up_v, in_sem.at[1])
    get_gate.start()
    get_up.start()

    def get_w(j):
        cols = pl.ds(pl.multiple_of(j * TILE, TILE), TILE)
        return pltpu.make_async_copy(w_hbm.at[:, cols], w_v.at[pl.ds(0, K), cols], w_sem.at[j])

    sibling = {"c": 1 - core}
    across = {"l": 1 - lo}
    diagonal = {"l": 1 - lo, "c": 1 - core}
    partners = [sibling, across, diagonal, ring("y", y, 2)]
    for axis, index in (("x", x), ("y", y), ("h", hi)):
        partners += [ring(axis, index, 1), ring(axis, index, 3)]

    barrier = pltpu.get_barrier_semaphore()
    for who in partners:
        pl.semaphore_signal(barrier, inc=1, device_id=who, device_id_type=pl.DeviceIdType.MESH)

    for j in range(HX // TILE):
        get_w(j).start()
    w_v[K:, :] = jnp.zeros((KP - K, N), BF16)
    with scope("get_in"):
        get_gate.wait()
        get_up.wait()
    for j in range(HX // TILE, N // TILE):
        get_w(j).start()

    for k in range(KP // 128):
        depth = min(128, K - k * 128)
        g = gate_v[k * 128 : k * 128 + depth, :].astype(F32)
        u = up_v[k * 128 : k * 128 + depth, :].astype(F32)
        act = g / (1.0 + jnp.exp(-g)) * u
        if depth < 128:
            act = jnp.concatenate([act, jnp.zeros((128 - depth, 256), F32)], axis=0)
        h[0, :, k * 128 : (k + 1) * 128] = act.T.astype(BF16)

    with scope("barrier"):
        pl.semaphore_wait(barrier, len(partners))

    def remote(src, dst, send, recv, who):
        return pltpu.make_async_remote_copy(
            src_ref=src, dst_ref=dst, send_sem=send, recv_sem=recv,
            device_id=who, device_id_type=pl.DeviceIdType.MESH,
        )

    gathers = [
        remote(h.at[0], h.at[1], ag_send.at[0], ag_recv.at[0], sibling),
        remote(h.at[0], h.at[2], ag_send.at[1], ag_recv.at[1], across),
        remote(h.at[2], h.at[3], ag_send.at[2], ag_recv.at[2], sibling),
    ]
    gathers[1].start()
    gathers[0].start()

    blocks = (2 * lo + core, 2 * lo + 1 - core, 2 * (1 - lo) + core, 2 * (1 - lo) + 1 - core)
    roles = [lax.rem(b + 4 - y, 4) for b in blocks]

    def rows(index, step, size):
        return pl.ds(pl.multiple_of(lax.rem(index + step, 4) * size, size), size)

    low_x, high_x = pl.ds(0, HX), pl.ds(HX, HX)
    low_y, high_y = pl.ds(0, HY), pl.ds(HY, HY)
    x_ways, y_ways, h_ways = (
        (ring(a, index, 1), ring(a, index, 3)) for a, index in (("x", x), ("y", y), ("h", hi))
    )

    def message(kind, sources, targets, send, recv, ways):
        return remote(sources[kind](), targets[kind](), send, recv, ways[kind % 2])

    def x1(kind, i):
        return message(
            kind,
            (
                lambda: p16_x.at[i, rows(x, 2, 64), low_x],
                lambda: p16_x.at[i, rows(x, 2, 64), high_x],
                lambda: p16_x.at[i, rows(x, 1, 64), high_x],
                lambda: p16_x.at[i, rows(x, 3, 64), low_x],
                lambda: c_x.at[0, i],
                lambda: c_x.at[1, i],
            ),
            [lambda k=k: (ra_x, rb_x, rc_x)[k // 2].at[k % 2, i] for k in range(6)],
            s1_send.at[0, kind, i], s1_recv.at[0, kind, i], x_ways,
        )

    def y1(kind, i):
        return message(
            kind,
            (
                lambda: p16_y.at[i, 2, :, :, :, low_y],
                lambda: p16_y.at[i, 2, :, :, :, high_y],
                lambda: p16_y.at[i, 1, :, :, :, high_y],
                lambda: p16_y.at[i, 3, :, :, :, low_y],
                lambda: c_y.at[0, i],
                lambda: c_y.at[1, i],
            ),
            [lambda k=k: (ra_y, rb_y, rc_y)[k // 2].at[k % 2, i] for k in range(6)],
            s1_send.at[1, kind, i], s1_recv.at[1, kind, i], y_ways,
        )

    def x2(kind, i):
        mine = rows(x, 0, 64)
        return message(
            kind,
            (
                lambda: p16_x.at[i, mine, low_x],
                lambda: p16_x.at[i, mine, high_x],
                lambda: p16_x.at[i, mine, high_x],
                lambda: p16_x.at[i, mine, low_x],
                lambda: c2_x.at[0],
                lambda: c2_x.at[1],
            ),
            [lambda k=k: r2_x.at[k] for k in range(6)],
            sx2_send.at[kind], sx2_recv.at[kind], y_ways,
        )

    def y2(kind, i):
        return message(
            kind,
            (
                lambda: p16_y.at[i, 0, :, lax.rem(hi + 2, 4), :, low_y],
                lambda: p16_y.at[i, 0, :, lax.rem(hi + 2, 4), :, high_y],
                lambda: p16_y.at[i, 0, :, lax.rem(hi + 1, 4), :, high_y],
                lambda: p16_y.at[i, 0, :, lax.rem(hi + 3, 4), :, low_y],
                lambda: c2_y.at[0, i],
                lambda: c2_y.at[1, i],
            ),
            [lambda k=k: r2_y.at[k, i] for k in range(6)],
            sy2_send.at[kind, i], sy2_recv.at[kind, i], h_ways,
        )

    def x3(kind):
        return message(
            kind,
            (
                lambda: t16_x.at[rows(hi, 2, 16), low_x],
                lambda: t16_x.at[rows(hi, 2, 16), high_x],
                lambda: t16_x.at[rows(hi, 1, 16), high_x],
                lambda: t16_x.at[rows(hi, 3, 16), low_x],
                lambda: c3_x.at[0],
                lambda: c3_x.at[1],
            ),
            [lambda k=k: r3_x.at[k] for k in range(6)],
            sx3_send.at[kind], sx3_recv.at[kind], h_ways,
        )

    def y3(kind, g):
        pair = pl.ds(2 * g, 2)
        return message(
            kind,
            (
                lambda: t16_y.at[pair, lax.rem(x + 2, 4), :, low_y],
                lambda: t16_y.at[pair, lax.rem(x + 2, 4), :, high_y],
                lambda: t16_y.at[pair, lax.rem(x + 1, 4), :, high_y],
                lambda: t16_y.at[pair, lax.rem(x + 3, 4), :, low_y],
                lambda: c3_y.at[0, g],
                lambda: c3_y.at[1, g],
            ),
            [lambda k=k: r3_y.at[k, g] for k in range(6)],
            sy3_send.at[kind, g], sy3_recv.at[kind, g], x_ways,
        )

    def x_product(i, first=False):
        with scope(f"x_product{i}"):
            for half in range(2):

                def step(j, carry):
                    j = half * (HX // TILE) + j
                    if first:
                        get_w(j).wait()
                    cols = pl.ds(pl.multiple_of(j * TILE, TILE), TILE)
                    part = jnp.dot(h[i], w_v[:, cols], preferred_element_type=F32)
                    p32_x[i, :, cols] = part
                    p16_x[i, :, cols] = part.astype(BF16)
                    return carry

                lax.fori_loop(0, HX // TILE, step, 0)
                for kind in ((0, 3), (1, 2))[half]:
                    x1(kind, i).start()

    def y_product(i, first=False):
        with scope(f"y_product{i}"):

            def quarter(r):
                at = lax.rem(y + r, 4)
                if first:
                    get_w(WX // TILE + at).wait()
                cols = pl.ds(pl.multiple_of(WX + at * QY, QY), QY)
                part = jnp.dot(h[i], w_v[:, cols], preferred_element_type=F32).reshape(4, 4, 16, QY)
                p32_y[i, r] = part
                p16_y[i, r] = part.astype(BF16)

            quarter(2)
            for kind in (0, 1):
                y1(kind, i).start()
            lax.fori_loop(0, 3, lambda j, c: (quarter(lax.rem(5 - j, 4)), c)[1], 0)
            for kind in (2, 3):
                y1(kind, i).start()

    def x_relay(i):
        with scope(f"x_relay{i}"):
            for s, step in ((0, 1), (1, 3)):
                x1(s, i).wait_recv()
                mine = p32_x[i, rows(x, step, 64), s * HX : (s + 1) * HX]
                c_x[s, i] = (mine + ra_x[s, i].astype(F32)).astype(BF16)
                x1(4 + s, i).start()

    def y_relay(i):
        with scope(f"y_relay{i}"):
            for s, r in ((0, 1), (1, 3)):
                y1(s, i).wait_recv()
                mine = p32_y[i, r, :, :, :, s * HY : (s + 1) * HY]
                c_y[s, i] = (mine + ra_y[s, i].astype(F32)).astype(BF16)
                y1(4 + s, i).start()

    def x_finish(i):
        with scope(f"x_finish{i}"):
            for kind in (2, 3, 4, 5):
                x1(kind, i).wait_recv()
            mine = rows(x, 0, 64)
            for s, (a, b) in ((0, (rc_x[0, i], rb_x[1, i])), (1, (rb_x[0, i], rc_x[1, i]))):
                cols = pl.ds(s * HX, HX)
                total = p32_x[i, mine, cols] + a.astype(F32) + b.astype(F32)
                p32_x[i, mine, cols] = total
                p16_x[i, mine, cols] = total.astype(BF16)
            for r, kinds in ((2, (0, 1)), (1, (2,)), (3, (3,))):

                @pl.when(roles[i] == r)
                def _():
                    for kind in kinds:
                        x2(kind, i).start()

    def y_finish(i):
        with scope(f"y_finish{i}"):
            for kind in (2, 3, 4, 5):
                y1(kind, i).wait_recv()
            for s, (a, b) in ((0, (rc_y[0, i], rb_y[1, i])), (1, (rb_y[0, i], rc_y[1, i]))):
                cols = pl.ds(s * HY, HY)
                total = p32_y[i, 0, :, :, :, cols] + a.astype(F32) + b.astype(F32)
                p32_y[i, 0, :, :, :, cols] = total
                p16_y[i, 0, :, :, :, cols] = total.astype(BF16)
            for kind in (0, 1, 2, 3):
                y2(kind, i).start()

    def x_relay2(i):
        with scope(f"x_second{i}"):
            for s, r in ((0, 1), (1, 3)):

                @pl.when(roles[i] == r)
                def _():
                    x2(s, i).wait_recv()
                    mine = p32_x[i, rows(x, 0, 64), s * HX : (s + 1) * HX]
                    c2_x[s] = (mine + r2_x[s].astype(F32)).astype(BF16)
                    x2(4 + s, i).start()

    def y_relay2(i):
        with scope(f"y_second{i}"):
            for s, step in ((0, 1), (1, 3)):
                y2(s, i).wait_recv()
                mine = p32_y[i, 0, :, lax.rem(hi + step, 4), :, s * HY : (s + 1) * HY]
                c2_y[s, i] = (mine + r2_y[s, i].astype(F32)).astype(BF16)
                y2(4 + s, i).start()

    def x_finish2(i):
        with scope("x_finish_second"):
            for kind in (2, 3, 4, 5):
                x2(kind, i).wait_recv()
            for s, (a, b) in ((0, (4, 3)), (1, (2, 5))):
                cols = pl.ds(s * HX, HX)
                total = p32_x[i, rows(x, 0, 64), cols] + r2_x[a].astype(F32) + r2_x[b].astype(F32)
                t32_x[:, cols] = total
                t16_x[:, cols] = total.astype(LAST_X)
            for kind in (0, 1, 2, 3):
                x3(kind).start()

    def y_finish2(g):
        with scope(f"y_finish_second{g}"):
            for i in (2 * g, 2 * g + 1):
                for kind in (2, 3, 4, 5):
                    y2(kind, i).wait_recv()
                for s, (a, b) in ((0, (4, 3)), (1, (2, 5))):
                    cols = pl.ds(s * HY, HY)
                    total = p32_y[i, 0, :, hi, :, cols] + r2_y[a, i].astype(F32) + r2_y[b, i].astype(F32)
                    t32_y[i, :, :, cols] = total
                    t16_y[i, :, :, cols] = total.astype(LAST_Y)
            for kind in (0, 1, 2, 3):
                y3(kind, g).start()

    def x_relay3():
        with scope("x_third"):
            for s in range(2):
                x3(s).wait_recv()
                mine = t32_x[rows(hi, 1 + 2 * s, 16), s * HX : (s + 1) * HX]
                c3_x[s] = (mine + r3_x[s].astype(F32)).astype(LAST_X)
                x3(4 + s).start()

    def y_relay3(g):
        with scope(f"y_third{g}"):
            for s in range(2):
                y3(s, g).wait_recv()
                mine = t32_y[2 * g : 2 * g + 2, lax.rem(x + 1 + 2 * s, 4), :, s * HY : (s + 1) * HY]
                c3_y[s, g] = (mine + r3_y[s, g].astype(F32)).astype(LAST_Y)
                y3(4 + s, g).start()

    def turn(i):
        d = lax.rem(y + 4 - blocks[i], 4)
        return remote(u_y.at[i], turned.at[d], turn_send.at[i], turn_recv.at[d], {"y": blocks[i]})

    def y_finish3(g):
        with scope(f"y_finish_third{g}"):
            for kind in (2, 3, 4, 5):
                y3(kind, g).wait_recv()
            for i in (2 * g, 2 * g + 1):
                for s, (a, b) in ((0, (4, 3)), (1, (2, 5))):
                    cols = pl.ds(s * HY, HY)
                    total = t32_y[i, x, :, cols]
                    total = total + r3_y[a, g, i % 2].astype(F32) + r3_y[b, g, i % 2].astype(F32)
                    u_y[i, :, cols] = total

                @pl.when(roles[i] != 0)
                def _():
                    turn(i).start()

    def folded(value):
        total = value[:, :128]
        for j in range(1, value.shape[1] // 128):
            total = total + value[:, j * 128 : (j + 1) * 128]
        return total

    def x_finish3():
        with scope("x_finish_third"):
            for kind in (2, 3, 4, 5):
                x3(kind).wait_recv()
            squares = jnp.zeros((16, 128), F32)
            for s, (a, b) in ((0, (4, 3)), (1, (2, 5))):
                cols = pl.ds(s * HX, HX)
                total = t32_x[rows(hi, 0, 16), cols] + r3_x[a].astype(F32) + r3_x[b].astype(F32)
                total = total + res_ref[:, cols].astype(F32)
                summed[:, cols] = total
                out_ref[0, :, cols] = total.astype(BF16)
                squares = squares + folded(total * total)
            return squares

    def y_close(squares):
        with scope("y_close"):
            own = 2 * lax.rem(y // 2 + lo, 2) + lax.rem(y + core, 2)
            for d in range(4):
                if d:
                    turn_in = remote(
                        turned.at[d], turned.at[d], turn_send.at[0], turn_recv.at[d], {"y": lax.rem(y + d, 4)}
                    )
                    turn_in.wait_recv()
                value = turned[d] if d else u_y[own]
                cols = pl.ds(pl.multiple_of(WX + lax.rem(y + d, 4) * QY, QY), QY)
                total = value + res_ref[:, cols].astype(F32)
                summed[:, cols] = total
                out_ref[0, :, cols] = total.astype(BF16)
                squares = squares + folded(total * total)
            return squares

    x_product(0, first=True)
    y_product(0, first=True)
    with scope("gather0"):
        gathers[0].wait_recv()
    x_product(1)
    y_product(1)
    x_relay(0)
    y_relay(0)
    with scope("gather1"):
        gathers[1].wait_recv()
    gathers[2].start()
    y_product(2)
    x_product(2)
    x_relay(1)
    y_relay(1)
    with scope("gather2"):
        gathers[2].wait_recv()
    y_product(3)
    x_product(3)
    y_finish(0)
    x_finish(0)
    y_relay(2)
    x_relay(2)
    y_finish(1)
    x_finish(1)
    y_relay2(0)
    x_relay2(0)
    y_relay(3)
    x_relay(3)
    y_relay2(1)
    x_relay2(1)
    y_finish2(0)
    y_finish(2)
    x_finish(2)
    y_finish(3)
    x_finish(3)
    y_relay3(0)
    y_relay2(2)
    x_relay2(2)
    y_relay2(3)
    x_relay2(3)
    y_finish3(0)
    own_slot = 2 * lax.rem(y // 2 + lo, 2) + lax.rem(y + core, 2)
    y_finish2(1)
    x_finish2(own_slot)
    y_relay3(1)
    x_relay3()
    y_finish3(1)
    total = y_close(x_finish3())

    sq_own[...] = total
    exchange = [
        remote(sq_own, sq_in.at[i], n_send.at[i], n_recv.at[i], who)
        for i, who in enumerate((sibling, across, diagonal))
    ]
    for copy in exchange:
        copy.start()
    with scope("drain"):
        for copy in gathers:
            copy.wait_send()
        for kind in range(6):
            for i in range(4):
                x1(kind, i).wait_send()
                y1(kind, i).wait_send()
                y2(kind, i).wait_send()
            x2(kind, 0).wait_send()
            x3(kind).wait_send()
            for g in range(2):
                y3(kind, g).wait_send()
        for i in range(4):

            @pl.when(roles[i] != 0)
            def _():
                turn(i).wait_send()

    with scope("exchange"):
        for copy in exchange:
            copy.wait_recv()
    for i in range(3):
        total = total + sq_in[i]
    scale = lax.rsqrt(jnp.sum(total, axis=1, keepdims=True) / D + 1e-05)
    for j in range(N // 128):
        cols = pl.ds(j * 128, 128)
        out_ref[1, :, cols] = (summed[:, cols] * scale * gain_ref[j : j + 1, :].astype(F32)).astype(BF16)
    for copy in exchange:
        copy.wait_send()


def body(gate_in, up_in, down_weight, residual, norm_gain):
    dma = pltpu.SemaphoreType.DMA
    vm = pltpu.VMEM
    scratch = [vm((K, 256), BF16), vm((K, 256), BF16), vm((KP, N), BF16), vm((4, 256, KP), BF16)]
    scratch += [vm((4, 256, WX), F32), vm((4, 256, WX), BF16)]
    scratch += [vm((4, 4, 4, 4, 16, QY), F32), vm((4, 4, 4, 4, 16, QY), BF16)]
    scratch += [vm((2, 4, 64, HX), BF16)] * 4 + [vm((2, 4, 4, 4, 16, HY), BF16)] * 4
    scratch += [vm((6, 64, HX), BF16), vm((2, 64, HX), BF16), vm((6, 4, 4, 16, HY), BF16), vm((2, 4, 4, 16, HY), BF16)]
    scratch += [vm((64, WX), F32), vm((64, WX), LAST_X), vm((4, 4, 16, QY), F32), vm((4, 4, 16, QY), LAST_Y)]
    scratch += [vm((6, 16, HX), LAST_X), vm((2, 16, HX), LAST_X)]
    scratch += [vm((6, 2, 2, 16, HY), LAST_Y), vm((2, 2, 2, 16, HY), LAST_Y)]
    scratch += [vm((4, 16, QY), F32), vm((4, 16, QY), F32), vm((16, N), F32), vm((16, 128), F32), vm((3, 16, 128), F32)]
    sems = [(2,), (N // TILE,), (3,), (3,), (2, 6, 4), (2, 6, 4), (6,), (6,), (6, 4), (6, 4)]
    sems += [(6,), (6,), (6, 2), (6, 2), (4,), (4,), (3,), (3,)]
    scratch += [dma(shape) for shape in sems]
    anywhere = pl.BlockSpec(memory_space=pl.ANY)
    vmem = pl.BlockSpec(memory_space=pltpu.VMEM)
    both = pl.pallas_call(
        kernel,
        out_shape=jax.ShapeDtypeStruct((2, 16, N), BF16),
        in_specs=[anywhere, anywhere, anywhere, vmem, vmem],
        out_specs=vmem,
        scratch_shapes=scratch,
        compiler_params=pltpu.CompilerParams(
            collective_id=0, has_side_effects=True, vmem_limit_bytes=VMEM_LIMIT
        ),
    )(gate_in.T, up_in.T, down_weight, residual, norm_gain.reshape(N // 128, 128))
    return both[0], both[1]


def solution(mesh):
    split = Mesh(mesh.devices.reshape(4, 4, 4, 2, 2), ("y", "x", "h", "l", "c"))
    tp, col = ("y", "x", "h"), ("l", "c")
    return jax.shard_map(
        body,
        mesh=split,
        in_specs=(P(col, tp), P(col, tp), P(tp, col), P(tp, col), P(col)),
        out_specs=(P(tp, col), P(tp, col)),
        check_vma=False,
    )
```

```python
import functools

import jax
import jax.numpy as jnp
from jax import lax
from jax.experimental import pallas as pl
from jax.experimental.pallas import tpu as pltpu
from jax.sharding import Mesh
from jax.sharding import PartitionSpec as P

F32 = jnp.float32
BF16 = jnp.bfloat16
D = 16384
N = 4096
K = 832
KP = 896
TILE = 512
VMEM_LIMIT = 58 * 1024 * 1024
WX = 2048
WY = N - WX
HX, QY = WX // 2, WY // 4
HY = QY // 2
LAST_X = BF16
LAST_Y = F32


def kernel(
    gate_hbm, up_hbm, w_hbm, res_hbm, gain_hbm, out_ref,
    gate_v, up_v, res_ref, gain_ref, w_v, h,
    p32_x, p16_x, p32_y, p16_y,
    a1_x, bc1_x, c1_x, a1_y, bc1_y, c1_y,
    a2_x, bc2_x, c2_x, a2_y, bc2_y, c2_y,
    t32_x, t16_x, t32_y, t16_y,
    line, plane,
    summed, sq_own, sq_in,
    in_sem, w_sem, ag_send, ag_recv, send_sem, a1_recv, bc1_recv, a2_recv, bc2_recv, last_recv, n_sem,
):
    x, y, hi, lo, core = (lax.axis_index(a) for a in ("x", "y", "h", "l", "c"))
    scope = jax.named_scope

    def ring(axis, index, step):
        return {axis: lax.rem(index + step, 4)}

    get_gate = pltpu.make_async_copy(gate_hbm, gate_v, in_sem.at[0])
    get_up = pltpu.make_async_copy(up_hbm, up_v, in_sem.at[1])
    get_gate.start()
    get_up.start()

    def get_w(j):
        cols = pl.ds(pl.multiple_of(j * TILE, TILE), TILE)
        return pltpu.make_async_copy(w_hbm.at[:, cols], w_v.at[pl.ds(0, K), cols], w_sem.at[j])

    sibling = {"c": 1 - core}
    across = {"l": 1 - lo}
    diagonal = {"l": 1 - lo, "c": 1 - core}
    partners = [sibling, across, diagonal]
    partners += [ring("h", hi, 1), ring("h", hi, 3)]
    partners += [ring("y", y, d) | ring("x", x, e) for d in range(4) for e in range(4) if d + e]

    barrier = pltpu.get_barrier_semaphore()
    for who in partners:
        pl.semaphore_signal(barrier, inc=1, device_id=who, device_id_type=pl.DeviceIdType.MESH)

    for j in range(HX // TILE):
        get_w(j).start()
    w_v[K:, :] = jnp.zeros((KP - K, N), BF16)
    with scope("get_in"):
        get_gate.wait()
        get_up.wait()
    for j in range(HX // TILE, N // TILE):
        get_w(j).start()
    get_rest = [
        pltpu.make_async_copy(res_hbm, res_ref, in_sem.at[2]),
        pltpu.make_async_copy(gain_hbm, gain_ref, in_sem.at[3]),
    ]
    for copy in get_rest:
        copy.start()

    for k in range(KP // 128):
        depth = min(128, K - k * 128)
        g = gate_v[k * 128 : k * 128 + depth, :].astype(F32)
        u = up_v[k * 128 : k * 128 + depth, :].astype(F32)
        act = g / (1.0 + jnp.exp(-g)) * u
        if depth < 128:
            act = jnp.concatenate([act, jnp.zeros((128 - depth, 256), F32)], axis=0)
        h[0, :, k * 128 : (k + 1) * 128] = act.T.astype(BF16)

    with scope("barrier"):
        pl.semaphore_wait(barrier, len(partners))

    def remote(src, dst, send, recv, who):
        return pltpu.make_async_remote_copy(
            src_ref=src, dst_ref=dst, send_sem=send, recv_sem=recv,
            device_id=who, device_id_type=pl.DeviceIdType.MESH,
        )

    gathers = [
        remote(h.at[0], h.at[1], ag_send, ag_recv.at[0], sibling),
        remote(h.at[0], h.at[2], ag_send, ag_recv.at[1], across),
        remote(h.at[2], h.at[3], ag_send, ag_recv.at[2], sibling),
    ]
    gathers[1].start()
    gathers[0].start()

    blocks = (2 * lo + core, 2 * lo + 1 - core, 2 * (1 - lo) + core, 2 * (1 - lo) + 1 - core)
    roles = [lax.rem(b + 4 - y, 4) for b in blocks]

    def rows(index, step, size):
        return pl.ds(pl.multiple_of(lax.rem(index + step, 4) * size, size), size)

    low_x, high_x = pl.ds(0, HX), pl.ds(HX, HX)
    low_y, high_y = pl.ds(0, HY), pl.ds(HY, HY)
    x_ways, y_ways, h_ways = (
        (ring(a, index, 1), ring(a, index, 3)) for a, index in (("x", x), ("y", y), ("h", hi))
    )

    def message(stage, colour, kind, i, source):
        a, bc, ways = buffers[stage][colour]
        a_recv, bc_recv = ((a1_recv, bc1_recv), (a2_recv, bc2_recv))[stage]
        if kind < 2:
            target, recv = a.at[kind, i], a_recv.at[colour, kind, i]
        else:
            target, recv = bc.at[i, kind - 2], bc_recv.at[colour, i]
        return remote(source, target, send_sem.at[stage, colour, kind // 4], recv, ways[kind % 2])

    buffers = (((a1_x, bc1_x, x_ways), (a1_y, bc1_y, y_ways)), ((a2_x, bc2_x, h_ways), (a2_y, bc2_y, h_ways)))

    def arrived(ref, sem):
        remote(ref, ref, sem, sem, sibling).wait_recv()

    def x1(kind, i):
        step, cols = ((2, low_x), (2, high_x), (1, high_x), (3, low_x), (0, None), (0, None))[kind]
        source = p16_x.at[i, rows(x, step, 64), cols] if kind < 4 else c1_x.at[kind - 4, i]
        return message(0, 0, kind, i, source)

    def y1(kind, i):
        step, cols = ((2, low_y), (2, high_y), (1, high_y), (3, low_y), (0, None), (0, None))[kind]
        source = p16_y.at[i, step, :, :, :, cols] if kind < 4 else c1_y.at[kind - 4, i]
        return message(0, 1, kind, i, source)

    def mine(step):
        return pl.ds(pl.multiple_of(x * 64 + lax.rem(hi + step, 4) * 16, 16), 16)

    def x2(kind, i):
        step, cols = ((2, low_x), (2, high_x), (1, high_x), (3, low_x), (0, None), (0, None))[kind]
        source = p16_x.at[i, mine(step), cols] if kind < 4 else c2_x.at[kind - 4, i]
        return message(1, 0, kind, i, source)

    def y2(kind, i):
        step, cols = ((2, low_y), (2, high_y), (1, high_y), (3, low_y), (0, None), (0, None))[kind]
        source = p16_y.at[i, 0, :, lax.rem(hi + step, 4), :, cols] if kind < 4 else c2_y.at[kind - 4, i]
        return message(1, 1, kind, i, source)

    def line_message(i):
        d = lax.rem(4 - roles[i], 4)
        return remote(t16_x.at[i], line.at[d], send_sem.at[2, 0, 0], last_recv.at[0], {"y": blocks[i]})

    def plane_message(i, e):
        d = lax.rem(4 - roles[i], 4)
        to = lax.rem(x + e, 4)
        n = 1 if e else 0
        return remote(
            t16_y.at[i, to], plane.at[d, (4 - e) % 4], send_sem.at[2, 1, n], last_recv.at[1 + n],
            {"y": blocks[i], "x": to},
        )

    def x_product(i, first=False):
        with scope(f"x_product{i}"):
            for half in range(2):

                def step(j, carry):
                    j = half * (HX // TILE) + j
                    if first:
                        get_w(j).wait()
                    cols = pl.ds(pl.multiple_of(j * TILE, TILE), TILE)
                    part = jnp.dot(h[i], w_v[:, cols], preferred_element_type=F32)
                    p32_x[i, :, cols] = part
                    p16_x[i, :, cols] = part.astype(BF16)
                    return carry

                lax.fori_loop(0, HX // TILE, step, 0)
                for kind in ((0, 3), (1, 2))[half]:
                    x1(kind, i).start()

    def y_product(i, first=False):
        with scope(f"y_product{i}"):

            def quarter(r):
                at = lax.rem(y + r, 4)
                if first:
                    get_w(WX // TILE + at).wait()
                cols = pl.ds(pl.multiple_of(WX + at * QY, QY), QY)
                part = jnp.dot(h[i], w_v[:, cols], preferred_element_type=F32).reshape(4, 4, 16, QY)
                p32_y[i, r] = part
                p16_y[i, r] = part.astype(BF16)

            quarter(2)
            for kind in (0, 1):
                y1(kind, i).start()
            lax.fori_loop(0, 3, lambda j, c: (quarter(lax.rem(5 - j, 4)), c)[1], 0)
            for kind in (2, 3):
                y1(kind, i).start()

    def x_relay(i):
        with scope(f"x_relay{i}"):
            for s, step in ((0, 1), (1, 3)):
                arrived(a1_x.at[s, i], a1_recv.at[0, s, i])
                own = p32_x[i, rows(x, step, 64), s * HX : (s + 1) * HX]
                c1_x[s, i] = (own + a1_x[s, i].astype(F32)).astype(BF16)
                x1(4 + s, i).start()

    def y_relay(i):
        with scope(f"y_relay{i}"):
            for s, r in ((0, 1), (1, 3)):
                arrived(a1_y.at[s, i], a1_recv.at[1, s, i])
                own = p32_y[i, r, :, :, :, s * HY : (s + 1) * HY]
                c1_y[s, i] = (own + a1_y[s, i].astype(F32)).astype(BF16)
                y1(4 + s, i).start()

    halves = ((2, 1), (0, 3))

    def x_finish(i):
        with scope(f"x_finish{i}"):
            arrived(bc1_x.at[i], bc1_recv.at[0, i])
            own = rows(x, 0, 64)
            for s, (a, b) in enumerate(halves):
                cols = pl.ds(s * HX, HX)
                total = p32_x[i, own, cols] + bc1_x[i, a].astype(F32) + bc1_x[i, b].astype(F32)
                p32_x[i, own, cols] = total
                p16_x[i, own, cols] = total.astype(BF16)
            for kind in (0, 1, 2, 3):
                x2(kind, i).start()

    def y_finish(i):
        with scope(f"y_finish{i}"):
            arrived(bc1_y.at[i], bc1_recv.at[1, i])
            for s, (a, b) in enumerate(halves):
                cols = pl.ds(s * HY, HY)
                total = p32_y[i, 0, :, :, :, cols] + bc1_y[i, a].astype(F32) + bc1_y[i, b].astype(F32)
                p32_y[i, 0, :, :, :, cols] = total
                p16_y[i, 0, :, :, :, cols] = total.astype(BF16)
            for kind in (0, 1, 2, 3):
                y2(kind, i).start()

    def x_relay2(i):
        with scope(f"x_second{i}"):
            for s, step in ((0, 1), (1, 3)):
                arrived(a2_x.at[s, i], a2_recv.at[0, s, i])
                own = p32_x[i, mine(step), s * HX : (s + 1) * HX]
                c2_x[s, i] = (own + a2_x[s, i].astype(F32)).astype(BF16)
                x2(4 + s, i).start()

    def y_relay2(i):
        with scope(f"y_second{i}"):
            for s, step in ((0, 1), (1, 3)):
                arrived(a2_y.at[s, i], a2_recv.at[1, s, i])
                own = p32_y[i, 0, :, lax.rem(hi + step, 4), :, s * HY : (s + 1) * HY]
                c2_y[s, i] = (own + a2_y[s, i].astype(F32)).astype(BF16)
                y2(4 + s, i).start()

    def x_finish2(i):
        with scope(f"x_finish_second{i}"):
            arrived(bc2_x.at[i], bc2_recv.at[0, i])
            for s, (a, b) in enumerate(halves):
                cols = pl.ds(s * HX, HX)
                total = p32_x[i, mine(0), cols] + bc2_x[i, a].astype(F32) + bc2_x[i, b].astype(F32)
                t32_x[i, :, cols] = total
                t16_x[i, :, cols] = total.astype(LAST_X)

            @pl.when(roles[i] != 0)
            def _():
                line_message(i).start()

    def y_finish2(i):
        with scope(f"y_finish_second{i}"):
            arrived(bc2_y.at[i], bc2_recv.at[1, i])
            for s, (a, b) in enumerate(halves):
                cols = pl.ds(s * HY, HY)
                total = p32_y[i, 0, :, hi, :, cols] + bc2_y[i, a].astype(F32) + bc2_y[i, b].astype(F32)
                t32_y[i, :, :, cols] = total
                t16_y[i, :, :, cols] = total.astype(LAST_Y)
            for e in (2, 1, 3):
                plane_message(i, e).start()

            @pl.when(roles[i] != 0)
            def _():
                plane_message(i, 0).start()

    def folded(value):
        total = value[:, :128]
        for j in range(1, value.shape[1] // 128):
            total = total + value[:, j * 128 : (j + 1) * 128]
        return total

    def close(total, cols, squares):
        total = total + res_ref[:, cols].astype(F32)
        summed[:, cols] = total
        out_ref[0, :, cols] = total.astype(BF16)
        return squares + folded(total * total)

    def x_close(squares):
        with scope("x_close"):
            arrived(line.at[pl.ds(1, 3)], last_recv.at[0])
            total = t32_x[own_slot]
            for d in (1, 2, 3):
                total = total + line[d].astype(F32)
            return close(total, pl.ds(0, WX), squares)

    def y_close(squares):
        with scope("y_close"):
            arrived(plane.at[pl.ds(1, 3), 0], last_recv.at[1])
            arrived(plane.at[:, pl.ds(1, 3)], last_recv.at[2])
            for d in range(4):
                total = plane[d, 0].astype(F32) if d else t32_y[own_slot, x]
                for e in (1, 2, 3):
                    total = total + plane[d, e].astype(F32)
                squares = close(total, pl.ds(pl.multiple_of(WX + lax.rem(y + d, 4) * QY, QY), QY), squares)
            return squares

    own_slot = 2 * lax.rem(y // 2 + lo, 2) + lax.rem(y + core, 2)
    y_product(0, first=True)
    x_product(0, first=True)
    y_relay(0)
    with scope("gather0"):
        gathers[0].wait_recv()
    y_product(1)
    x_relay(0)
    x_product(1)
    y_finish(0)
    x_finish(0)
    y_relay(1)
    with scope("gather1"):
        gathers[1].wait_recv()
    gathers[2].start()
    y_product(2)
    x_relay(1)
    with scope("gather2"):
        gathers[2].wait_recv()
    x_product(3)
    x_relay2(0)
    y_finish(1)
    x_finish(1)
    y_relay(2)
    y_relay2(0)
    y_product(3)
    y_relay2(1)
    x_relay(3)
    x_relay2(1)
    x_product(2)
    x_finish(3)
    y_finish(2)
    y_relay(3)
    x_finish2(1)
    x_relay2(3)
    x_relay(2)
    y_finish(3)
    x_finish2(0)
    x_finish(2)
    y_finish2(0)
    y_relay2(3)
    y_relay2(2)
    y_finish2(1)
    x_finish2(3)
    x_relay2(2)
    y_finish2(3)
    y_finish2(2)
    x_finish2(2)
    for copy in get_rest:
        copy.wait()
    total = y_close(x_close(jnp.zeros((16, 128), F32)))

    sq_own[...] = total
    exchange = [
        remote(sq_own, sq_in.at[i], n_sem.at[0], n_sem.at[1], who)
        for i, who in enumerate((sibling, across, diagonal))
    ]
    for copy in exchange:
        copy.start()
    with scope("drain"):
        arrived(h.at[pl.ds(0, 3)], ag_send)
        for colour, (bc1, c1, bc2, c2) in enumerate(((bc1_x, c1_x, bc2_x, c2_x), (bc1_y, c1_y, bc2_y, c2_y))):
            for stage, bc, c in ((0, bc1, c1), (1, bc2, c2)):
                arrived(bc, send_sem.at[stage, colour, 0])
                arrived(c, send_sem.at[stage, colour, 1])
        arrived(line.at[pl.ds(1, 3)], send_sem.at[2, 0, 0])
        arrived(plane.at[pl.ds(1, 3), 0], send_sem.at[2, 1, 0])
        arrived(plane.at[:, pl.ds(1, 3)], send_sem.at[2, 1, 1])

    with scope("exchange"):
        arrived(sq_in, n_sem.at[1])
    for i in range(3):
        total = total + sq_in[i]
    with scope("norm"):
        scale = lax.rsqrt(jnp.sum(total, axis=1, keepdims=True) / D + 1e-05)
        for j in range(N // 128):
            cols = pl.ds(j * 128, 128)
            out_ref[1, :, cols] = (summed[:, cols] * scale * gain_ref[j : j + 1, :].astype(F32)).astype(BF16)
    arrived(sq_in, n_sem.at[0])


def body(gate_in, up_in, down_weight, residual, norm_gain):
    dma = pltpu.SemaphoreType.DMA
    vm = pltpu.VMEM
    scratch = [vm((K, 256), BF16), vm((K, 256), BF16), vm((16, N), BF16), vm((N // 128, 128), BF16), vm((KP, N), BF16), vm((4, 256, KP), BF16)]
    scratch += [vm((4, 256, WX), F32), vm((4, 256, WX), BF16)]
    scratch += [vm((4, 4, 4, 4, 16, QY), F32), vm((4, 4, 4, 4, 16, QY), BF16)]
    for rows, cols in (((64,), HX), ((4, 4, 16), HY), ((16,), HX), ((4, 16), HY)):
        scratch += [vm((2, 4, *rows, cols), BF16), vm((4, 4, *rows, cols), BF16), vm((2, 4, *rows, cols), BF16)]
    scratch += [vm((4, 16, WX), F32), vm((4, 16, WX), LAST_X), vm((4, 4, 16, QY), F32), vm((4, 4, 16, QY), LAST_Y)]
    scratch += [vm((4, 16, WX), LAST_X), vm((4, 4, 16, QY), LAST_Y)]
    scratch += [vm((16, N), F32), vm((16, 128), F32), vm((3, 16, 128), F32)]
    scratch += [dma((4,)), dma((N // TILE,)), dma, dma((3,)), dma((3, 2, 2))]
    scratch += [dma((2, 2, 4)), dma((2, 4)), dma((2, 2, 4)), dma((2, 4)), dma((3,)), dma((2,))]
    anywhere = pl.BlockSpec(memory_space=pltpu.HBM)
    vmem = pl.BlockSpec(memory_space=pltpu.VMEM)
    both = pl.pallas_call(
        kernel,
        out_shape=jax.ShapeDtypeStruct((2, 16, N), BF16),
        in_specs=[anywhere] * 5,
        out_specs=vmem,
        scratch_shapes=scratch,
        compiler_params=pltpu.CompilerParams(
            collective_id=0, has_side_effects=True, vmem_limit_bytes=VMEM_LIMIT
        ),
    )(gate_in.T, up_in.T, down_weight, residual, norm_gain.reshape(N // 128, 128))
    return both[0], both[1]


def solution(mesh):
    split = Mesh(mesh.devices.reshape(4, 4, 4, 2, 2), ("y", "x", "h", "l", "c"))
    tp, col = ("y", "x", "h"), ("l", "c")
    return jax.shard_map(
        body,
        mesh=split,
        in_specs=(P(col, tp), P(col, tp), P(tp, col), P(tp, col), P(col)),
        out_specs=(P(tp, col), P(tp, col)),
        check_vma=False,
    )
```

```python
import functools

import jax
import jax.numpy as jnp
from jax import lax
from jax.experimental import pallas as pl
from jax.experimental.pallas import tpu as pltpu
from jax.sharding import Mesh
from jax.sharding import PartitionSpec as P

F32 = jnp.float32
BF16 = jnp.bfloat16
D = 16384
N = 4096
K = 832
KP = 896
TILE = 512
VMEM_LIMIT = 50 * 1024 * 1024
WX = 2048
WY = N - WX
HX, QY = WX // 2, WY // 4
HY = QY // 2
LAST_X = BF16
LAST_Y = F32


def kernel(
    gate_hbm, up_hbm, w_hbm, res_hbm, gain_hbm, out_ref,
    gate_v, up_v, res_ref, gain_ref, w_v, h,
    p32_x, p16_x, p32_y, p16_y,
    a1_x, bc1_x, c1_x, a1_y, bc1_y, c1_y,
    a2_x, bc2_x, c2_x, a2_y, bc2_y, c2_y,
    t32_x, t16_x, t32_y, t16_y,
    line, plane,
    summed, sq_own, sq_in,
    in_sem, w_sem, ag_send, ag_recv, send_sem, a1_recv, bc1_recv, a2_recv, bc2_recv, last_recv, n_sem,
):
    x, y, hi, lo, core = (lax.axis_index(a) for a in ("x", "y", "h", "l", "c"))
    scope = jax.named_scope

    def ring(axis, index, step):
        return {axis: lax.rem(index + step, 4)}

    get_gate = pltpu.make_async_copy(gate_hbm, gate_v, in_sem.at[0])
    get_up = pltpu.make_async_copy(up_hbm, up_v, in_sem.at[1])
    get_gate.start()
    get_up.start()

    def get_w(j):
        cols = pl.ds(pl.multiple_of(j * TILE, TILE), TILE)
        return pltpu.make_async_copy(w_hbm.at[:, cols], w_v.at[pl.ds(0, K), cols], w_sem.at[j])

    sibling = {"c": 1 - core}
    across = {"l": 1 - lo}
    diagonal = {"l": 1 - lo, "c": 1 - core}
    partners = [sibling, across, diagonal]
    partners += [ring("h", hi, 1), ring("h", hi, 3)]
    partners += [ring("y", y, d) | ring("x", x, e) for d in range(4) for e in range(4) if d + e]

    barrier = pltpu.get_barrier_semaphore()
    for who in partners:
        pl.semaphore_signal(barrier, inc=1, device_id=who, device_id_type=pl.DeviceIdType.MESH)

    for j in range(HX // TILE):
        get_w(j).start()
    w_v[K:, :] = jnp.zeros((KP - K, N), BF16)
    with scope("get_in"):
        get_gate.wait()
        get_up.wait()
    for j in range(HX // TILE, N // TILE):
        get_w(j).start()
    get_rest = [
        pltpu.make_async_copy(res_hbm, res_ref, in_sem.at[2]),
        pltpu.make_async_copy(gain_hbm, gain_ref, in_sem.at[3]),
    ]
    for copy in get_rest:
        copy.start()

    for k in range(KP // 128):
        depth = min(128, K - k * 128)
        g = gate_v[k * 128 : k * 128 + depth, :].astype(F32)
        u = up_v[k * 128 : k * 128 + depth, :].astype(F32)
        act = g / (1.0 + jnp.exp(-g)) * u
        if depth < 128:
            act = jnp.concatenate([act, jnp.zeros((128 - depth, 256), F32)], axis=0)
        h[0, :, k * 128 : (k + 1) * 128] = act.T.astype(BF16)

    with scope("barrier"):
        pl.semaphore_wait(barrier, len(partners))

    def remote(src, dst, send, recv, who):
        return pltpu.make_async_remote_copy(
            src_ref=src, dst_ref=dst, send_sem=send, recv_sem=recv,
            device_id=who, device_id_type=pl.DeviceIdType.MESH,
        )

    gathers = [
        remote(h.at[0], h.at[1], ag_send, ag_recv.at[0], sibling),
        remote(h.at[0], h.at[2], ag_send, ag_recv.at[1], across),
        remote(h.at[2], h.at[3], ag_send, ag_recv.at[2], sibling),
    ]
    gathers[1].start()
    gathers[0].start()

    blocks = (2 * lo + core, 2 * lo + 1 - core, 2 * (1 - lo) + core, 2 * (1 - lo) + 1 - core)
    roles = [lax.rem(b + 4 - y, 4) for b in blocks]

    def rows(index, step, size):
        return pl.ds(pl.multiple_of(lax.rem(index + step, 4) * size, size), size)

    low_x, high_x = pl.ds(0, HX), pl.ds(HX, HX)
    low_y, high_y = pl.ds(0, HY), pl.ds(HY, HY)
    x_ways, y_ways, h_ways = (
        (ring(a, index, 1), ring(a, index, 3)) for a, index in (("x", x), ("y", y), ("h", hi))
    )

    def message(stage, colour, kind, i, source):
        a, bc, ways = buffers[stage][colour]
        a_recv, bc_recv = ((a1_recv, bc1_recv), (a2_recv, bc2_recv))[stage]
        if kind < 2:
            target, recv = a.at[kind, i], a_recv.at[colour, kind, i]
        else:
            target, recv = bc.at[i, kind - 2], bc_recv.at[colour, i]
        return remote(source, target, send_sem.at[stage, colour, kind // 4], recv, ways[kind % 2])

    buffers = (((a1_x, bc1_x, x_ways), (a1_y, bc1_y, y_ways)), ((a2_x, bc2_x, h_ways), (a2_y, bc2_y, h_ways)))

    def arrived(ref, sem):
        remote(ref, ref, sem, sem, sibling).wait_recv()

    def x1(kind, i):
        step, cols = ((2, low_x), (2, high_x), (1, high_x), (3, low_x), (0, None), (0, None))[kind]
        source = p16_x.at[i, rows(x, step, 64), cols] if kind < 4 else c1_x.at[kind - 4, i]
        return message(0, 0, kind, i, source)

    def y1(kind, i):
        step, cols = ((2, low_y), (2, high_y), (1, high_y), (3, low_y), (0, None), (0, None))[kind]
        source = p16_y.at[i, step, :, :, :, cols] if kind < 4 else c1_y.at[kind - 4, i]
        return message(0, 1, kind, i, source)

    def mine(step):
        return pl.ds(pl.multiple_of(x * 64 + lax.rem(hi + step, 4) * 16, 16), 16)

    def x2(kind, i):
        step, cols = ((2, low_x), (2, high_x), (1, high_x), (3, low_x), (0, None), (0, None))[kind]
        source = p16_x.at[i, mine(step), cols] if kind < 4 else c2_x.at[kind - 4, i]
        return message(1, 0, kind, i, source)

    def y2(kind, i):
        step, cols = ((2, low_y), (2, high_y), (1, high_y), (3, low_y), (0, None), (0, None))[kind]
        source = p16_y.at[i, 0, :, lax.rem(hi + step, 4), :, cols] if kind < 4 else c2_y.at[kind - 4, i]
        return message(1, 1, kind, i, source)

    def line_message(i):
        d = lax.rem(4 - roles[i], 4)
        return remote(t16_x.at[i], line.at[d], send_sem.at[2, 0, 0], last_recv.at[0], {"y": blocks[i]})

    def plane_message(i, e):
        d = lax.rem(4 - roles[i], 4)
        to = lax.rem(x + e, 4)
        n = 1 if e else 0
        return remote(
            t16_y.at[i, to], plane.at[d, (4 - e) % 4], send_sem.at[2, 1, n], last_recv.at[1 + n],
            {"y": blocks[i], "x": to},
        )

    def x_half(i, half):
        def step(j, carry):
            j = half * (HX // TILE) + j
            if i == 0:
                get_w(j).wait()
            cols = pl.ds(pl.multiple_of(j * TILE, TILE), TILE)
            part = jnp.dot(h[i], w_v[:, cols], preferred_element_type=F32)
            p32_x[i, :, cols] = part
            p16_x[i, :, cols] = part.astype(BF16)
            return carry

        lax.fori_loop(0, HX // TILE, step, 0)

    def y_quarters(i, count):
        def step(j, carry):
            r = lax.rem(5 - j, 4) if count == 3 else 2
            at = lax.rem(y + r, 4)
            if i == 0:
                get_w(WX // TILE + at).wait()
            cols = pl.ds(pl.multiple_of(WX + at * QY, QY), QY)
            part = jnp.dot(h[i], w_v[:, cols], preferred_element_type=F32).reshape(4, 4, 16, QY)
            p32_y[i, r] = part
            p16_y[i, r] = part.astype(BF16)
            return carry

        lax.fori_loop(0, count, step, 0)

    def first_product():
        with scope("first_product"):
            y_quarters(0, 1)
            for kind in (0, 1):
                y1(kind, 0).start()
            for half, kinds in enumerate(((0, 3), (1, 2))):
                x_half(0, half)
                for kind in kinds:
                    x1(kind, 0).start()
            y_quarters(0, 3)
            for kind in (2, 3):
                y1(kind, 0).start()

    def x_product(i):
        with scope(f"x_product{i}"):
            x_half(i, 0)
            x_half(i, 1)
            for kind in (0, 1, 2, 3):
                x1(kind, i).start()

    def y_product(i):
        with scope(f"y_product{i}"):
            y_quarters(i, 1)
            for kind in (0, 1):
                y1(kind, i).start()
            y_quarters(i, 3)
            for kind in (2, 3):
                y1(kind, i).start()

    def x_relay(i):
        with scope(f"x_relay{i}"):
            for s, step in ((0, 1), (1, 3)):
                arrived(a1_x.at[s, i], a1_recv.at[0, s, i])
                own = p32_x[i, rows(x, step, 64), s * HX : (s + 1) * HX]
                c1_x[s, i] = (own + a1_x[s, i].astype(F32)).astype(BF16)
                x1(4 + s, i).start()

    def y_relay(i):
        with scope(f"y_relay{i}"):
            for s, r in ((0, 1), (1, 3)):
                arrived(a1_y.at[s, i], a1_recv.at[1, s, i])
                own = p32_y[i, r, :, :, :, s * HY : (s + 1) * HY]
                c1_y[s, i] = (own + a1_y[s, i].astype(F32)).astype(BF16)
                y1(4 + s, i).start()

    halves = ((2, 1), (0, 3))

    def x_finish(i):
        with scope(f"x_finish{i}"):
            arrived(bc1_x.at[i], bc1_recv.at[0, i])
            own = rows(x, 0, 64)
            for s, (a, b) in enumerate(halves):
                cols = pl.ds(s * HX, HX)
                total = p32_x[i, own, cols] + bc1_x[i, a].astype(F32) + bc1_x[i, b].astype(F32)
                p32_x[i, own, cols] = total
                p16_x[i, own, cols] = total.astype(BF16)
            for kind in (0, 1, 2, 3):
                x2(kind, i).start()

    def y_finish(i):
        with scope(f"y_finish{i}"):
            arrived(bc1_y.at[i], bc1_recv.at[1, i])
            for s, (a, b) in enumerate(halves):
                cols = pl.ds(s * HY, HY)
                total = p32_y[i, 0, :, :, :, cols] + bc1_y[i, a].astype(F32) + bc1_y[i, b].astype(F32)
                p32_y[i, 0, :, :, :, cols] = total
                p16_y[i, 0, :, :, :, cols] = total.astype(BF16)
            for kind in (0, 1, 2, 3):
                y2(kind, i).start()

    def x_relay2(i):
        with scope(f"x_second{i}"):
            for s, step in ((0, 1), (1, 3)):
                arrived(a2_x.at[s, i], a2_recv.at[0, s, i])
                own = p32_x[i, mine(step), s * HX : (s + 1) * HX]
                c2_x[s, i] = (own + a2_x[s, i].astype(F32)).astype(BF16)
                x2(4 + s, i).start()

    def y_relay2(i):
        with scope(f"y_second{i}"):
            for s, step in ((0, 1), (1, 3)):
                arrived(a2_y.at[s, i], a2_recv.at[1, s, i])
                own = p32_y[i, 0, :, lax.rem(hi + step, 4), :, s * HY : (s + 1) * HY]
                c2_y[s, i] = (own + a2_y[s, i].astype(F32)).astype(BF16)
                y2(4 + s, i).start()

    def x_finish2(i):
        with scope(f"x_finish_second{i}"):
            arrived(bc2_x.at[i], bc2_recv.at[0, i])
            for s, (a, b) in enumerate(halves):
                cols = pl.ds(s * HX, HX)
                total = p32_x[i, mine(0), cols] + bc2_x[i, a].astype(F32) + bc2_x[i, b].astype(F32)
                t32_x[i, :, cols] = total
                t16_x[i, :, cols] = total.astype(LAST_X)

            @pl.when(roles[i] != 0)
            def _():
                line_message(i).start()

    def y_finish2(i):
        with scope(f"y_finish_second{i}"):
            arrived(bc2_y.at[i], bc2_recv.at[1, i])
            for s, (a, b) in enumerate(halves):
                cols = pl.ds(s * HY, HY)
                total = p32_y[i, 0, :, hi, :, cols] + bc2_y[i, a].astype(F32) + bc2_y[i, b].astype(F32)
                t32_y[i, :, :, cols] = total
                t16_y[i, :, :, cols] = total.astype(LAST_Y)
            for e in (2, 1, 3):
                plane_message(i, e).start()

            @pl.when(roles[i] != 0)
            def _():
                plane_message(i, 0).start()

    def folded(value):
        total = value[:, :128]
        for j in range(1, value.shape[1] // 128):
            total = total + value[:, j * 128 : (j + 1) * 128]
        return total

    def close(total, cols, squares):
        total = total + res_ref[:, cols].astype(F32)
        summed[:, cols] = total
        out_ref[0, :, cols] = total.astype(BF16)
        return squares + folded(total * total)

    def x_close(squares):
        with scope("x_close"):
            arrived(line.at[pl.ds(1, 3)], last_recv.at[0])
            total = t32_x[own_slot]
            for d in (1, 2, 3):
                total = total + line[d].astype(F32)
            return close(total, pl.ds(0, WX), squares)

    def y_close(squares):
        with scope("y_close"):
            arrived(plane.at[pl.ds(1, 3), 0], last_recv.at[1])
            arrived(plane.at[:, pl.ds(1, 3)], last_recv.at[2])
            for d in range(4):
                total = plane[d, 0].astype(F32) if d else t32_y[own_slot, x]
                for e in (1, 2, 3):
                    total = total + plane[d, e].astype(F32)
                squares = close(total, pl.ds(pl.multiple_of(WX + lax.rem(y + d, 4) * QY, QY), QY), squares)
            return squares

    own_slot = 2 * lax.rem(y // 2 + lo, 2) + lax.rem(y + core, 2)
    first_product()
    y_relay(0)
    with scope("gather0"):
        gathers[0].wait_recv()
    y_product(1)
    x_relay(0)
    x_product(1)
    y_finish(0)
    x_finish(0)
    y_relay(1)
    with scope("gather1"):
        gathers[1].wait_recv()
    gathers[2].start()
    y_product(2)
    x_relay(1)
    y_relay2(0)
    with scope("gather2"):
        gathers[2].wait_recv()
    x_product(3)
    x_relay2(0)
    y_finish(1)
    x_finish(1)
    y_relay(2)
    y_product(3)
    y_relay2(1)
    x_relay(3)
    x_product(2)
    x_relay2(1)
    y_finish(2)
    x_finish(3)
    y_relay(3)
    x_finish2(0)
    y_relay2(2)
    y_finish2(1)
    x_relay(2)
    x_finish2(1)
    x_relay2(3)
    y_finish(3)
    x_finish(2)
    y_relay2(3)
    y_finish2(0)
    y_finish2(2)
    x_relay2(2)
    x_finish2(3)
    y_finish2(3)
    x_finish2(2)
    for copy in get_rest:
        copy.wait()
    total = y_close(x_close(jnp.zeros((16, 128), F32)))

    sq_own[...] = total
    exchange = [
        remote(sq_own, sq_in.at[i], n_sem.at[0], n_sem.at[1], who)
        for i, who in enumerate((sibling, across, diagonal))
    ]
    for copy in exchange:
        copy.start()
    with scope("drain"):
        arrived(h.at[pl.ds(0, 3)], ag_send)
        for colour, (bc1, c1, bc2, c2) in enumerate(((bc1_x, c1_x, bc2_x, c2_x), (bc1_y, c1_y, bc2_y, c2_y))):
            for stage, bc, c in ((0, bc1, c1), (1, bc2, c2)):
                arrived(bc, send_sem.at[stage, colour, 0])
                arrived(c, send_sem.at[stage, colour, 1])
        arrived(line.at[pl.ds(1, 3)], send_sem.at[2, 0, 0])
        arrived(plane.at[pl.ds(1, 3), 0], send_sem.at[2, 1, 0])
        arrived(plane.at[:, pl.ds(1, 3)], send_sem.at[2, 1, 1])

    with scope("exchange"):
        arrived(sq_in, n_sem.at[1])
    for i in range(3):
        total = total + sq_in[i]
    with scope("norm"):
        scale = lax.rsqrt(jnp.sum(total, axis=1, keepdims=True) / D + 1e-05)
        for j in range(N // 128):
            cols = pl.ds(j * 128, 128)
            out_ref[1, :, cols] = (summed[:, cols] * scale * gain_ref[j : j + 1, :].astype(F32)).astype(BF16)
    arrived(sq_in, n_sem.at[0])


def body(gate_in, up_in, down_weight, residual, norm_gain):
    dma = pltpu.SemaphoreType.DMA
    vm = pltpu.VMEM
    scratch = [vm((K, 256), BF16), vm((K, 256), BF16), vm((16, N), BF16), vm((N // 128, 128), BF16), vm((KP, N), BF16), vm((4, 256, KP), BF16)]
    scratch += [vm((4, 256, WX), F32), vm((4, 256, WX), BF16)]
    scratch += [vm((4, 4, 4, 4, 16, QY), F32), vm((4, 4, 4, 4, 16, QY), BF16)]
    for rows, cols in (((64,), HX), ((4, 4, 16), HY), ((16,), HX), ((4, 16), HY)):
        scratch += [vm((2, 4, *rows, cols), BF16), vm((4, 4, *rows, cols), BF16), vm((2, 4, *rows, cols), BF16)]
    scratch += [vm((4, 16, WX), F32), vm((4, 16, WX), LAST_X), vm((4, 4, 16, QY), F32), vm((4, 4, 16, QY), LAST_Y)]
    scratch += [vm((4, 16, WX), LAST_X), vm((4, 4, 16, QY), LAST_Y)]
    scratch += [vm((16, N), F32), vm((16, 128), F32), vm((3, 16, 128), F32)]
    scratch += [dma((4,)), dma((N // TILE,)), dma, dma((3,)), dma((3, 2, 2))]
    scratch += [dma((2, 2, 4)), dma((2, 4)), dma((2, 2, 4)), dma((2, 4)), dma((3,)), dma((2,))]
    anywhere = pl.BlockSpec(memory_space=pltpu.HBM)
    vmem = pl.BlockSpec(memory_space=pltpu.VMEM)
    operands = (gate_in.T, up_in.T, down_weight, residual, norm_gain.reshape(N // 128, 128))
    operands = (pltpu.with_memory_space_constraint(a, pltpu.HBM) for a in operands)
    both = pl.pallas_call(
        kernel,
        out_shape=jax.ShapeDtypeStruct((2, 16, N), BF16),
        in_specs=[anywhere] * 5,
        out_specs=vmem,
        scratch_shapes=scratch,
        compiler_params=pltpu.CompilerParams(
            collective_id=0, has_side_effects=True, vmem_limit_bytes=VMEM_LIMIT
        ),
    )(*operands)
    return both[0], both[1]


def solution(mesh):
    split = Mesh(mesh.devices.reshape(4, 4, 4, 2, 2), ("y", "x", "h", "l", "c"))
    tp, col = ("y", "x", "h"), ("l", "c")
    return jax.shard_map(
        body,
        mesh=split,
        in_specs=(P(col, tp), P(col, tp), P(tp, col), P(tp, col), P(col)),
        out_specs=(P(tp, col), P(tp, col)),
        check_vma=False,
    )
```

```python
import functools

import jax
import jax.numpy as jnp
from jax import lax
from jax.experimental import pallas as pl
from jax.experimental.pallas import tpu as pltpu
from jax.sharding import Mesh
from jax.sharding import PartitionSpec as P

F32 = jnp.float32
BF16 = jnp.bfloat16
D = 16384
N = 4096
K = 832
KP = 896
TILE = 512
VMEM_LIMIT = 50 * 1024 * 1024
WX = 2048
WY = N - WX
HX, QY = WX // 2, WY // 4
HY = QY // 2
LAST_X = BF16
LAST_Y = BF16


def kernel(
    gate_hbm, up_hbm, w_hbm, res_hbm, gain_hbm, out_ref,
    gate_v, up_v, res_ref, gain_ref, w_v, h,
    p32_x, p16_x, p32_y, p16_y,
    a1_x, bc1_x, c1_x, a1_y, bc1_y, c1_y,
    a2_x, bc2_x, c2_x, a2_y, bc2_y, c2_y,
    t32_x, t16_x, t32_y, t16_y,
    line, plane,
    summed, sq_own, sq_in,
    in_sem, w_sem, ag_send, ag_recv, send_sem, a1_recv, bc1_recv, a2_recv, bc2_recv, last_recv, n_sem,
):
    x, y, hi, lo, core = (lax.axis_index(a) for a in ("x", "y", "h", "l", "c"))
    scope = jax.named_scope

    def ring(axis, index, step):
        return {axis: lax.rem(index + step, 4)}

    get_gate = pltpu.make_async_copy(gate_hbm, gate_v, in_sem.at[0])
    get_up = pltpu.make_async_copy(up_hbm, up_v, in_sem.at[1])
    get_gate.start()
    get_up.start()

    def get_w(j):
        cols = pl.ds(pl.multiple_of(j * TILE, TILE), TILE)
        return pltpu.make_async_copy(w_hbm.at[:, cols], w_v.at[pl.ds(0, K), cols], w_sem.at[j])

    sibling = {"c": 1 - core}
    across = {"l": 1 - lo}
    diagonal = {"l": 1 - lo, "c": 1 - core}
    partners = [sibling, across, diagonal]
    partners += [ring("h", hi, 1), ring("h", hi, 3)]
    partners += [ring("y", y, d) | ring("x", x, e) for d in range(4) for e in range(4) if d + e]

    barrier = pltpu.get_barrier_semaphore()
    for who in partners:
        pl.semaphore_signal(barrier, inc=1, device_id=who, device_id_type=pl.DeviceIdType.MESH)

    y_tile = WX // TILE
    for j in (y_tile + lax.rem(y + 2, 4), *range(HX // TILE)):
        get_w(j).start()
    w_v[K:, :] = jnp.zeros((KP - K, N), BF16)
    with scope("get_in"):
        get_gate.wait()
        get_up.wait()
    for j in (*range(HX // TILE, y_tile), *(y_tile + lax.rem(y + r, 4) for r in (1, 0, 3))):
        get_w(j).start()
    get_rest = [
        pltpu.make_async_copy(res_hbm, res_ref, in_sem.at[2]),
        pltpu.make_async_copy(gain_hbm, gain_ref, in_sem.at[3]),
    ]
    for copy in get_rest:
        copy.start()

    for k in range(KP // 128):
        depth = min(128, K - k * 128)
        g = gate_v[k * 128 : k * 128 + depth, :].astype(F32)
        u = up_v[k * 128 : k * 128 + depth, :].astype(F32)
        act = g / (1.0 + jnp.exp(-g)) * u
        if depth < 128:
            act = jnp.concatenate([act, jnp.zeros((128 - depth, 256), F32)], axis=0)
        h[0, :, k * 128 : (k + 1) * 128] = act.T.astype(BF16)

    def remote(src, dst, send, recv, who):
        return pltpu.make_async_remote_copy(
            src_ref=src, dst_ref=dst, send_sem=send, recv_sem=recv,
            device_id=who, device_id_type=pl.DeviceIdType.MESH,
        )

    gathers = [
        remote(h.at[0], h.at[1], ag_send, ag_recv.at[0], sibling),
        remote(h.at[0], h.at[2], ag_send, ag_recv.at[1], across),
        remote(h.at[2], h.at[3], ag_send, ag_recv.at[2], sibling),
    ]
    blocks = (2 * lo + core, 2 * lo + 1 - core, 2 * (1 - lo) + core, 2 * (1 - lo) + 1 - core)
    roles = [lax.rem(b + 4 - y, 4) for b in blocks]

    def rows(index, step, size):
        return pl.ds(pl.multiple_of(lax.rem(index + step, 4) * size, size), size)

    low_x, high_x = pl.ds(0, HX), pl.ds(HX, HX)
    low_y, high_y = pl.ds(0, HY), pl.ds(HY, HY)
    x_ways, y_ways, h_ways = (
        (ring(a, index, 1), ring(a, index, 3)) for a, index in (("x", x), ("y", y), ("h", hi))
    )

    def message(stage, colour, kind, i, source):
        a, bc, ways = buffers[stage][colour]
        a_recv, bc_recv = ((a1_recv, bc1_recv), (a2_recv, bc2_recv))[stage]
        if kind < 2:
            target, recv = a.at[kind, i], a_recv.at[colour, kind, i]
        else:
            target, recv = bc.at[i, kind - 2], bc_recv.at[colour, i]
        return remote(source, target, send_sem.at[stage, colour, kind // 4], recv, ways[kind % 2])

    buffers = (((a1_x, bc1_x, x_ways), (a1_y, bc1_y, y_ways)), ((a2_x, bc2_x, h_ways), (a2_y, bc2_y, h_ways)))

    def arrived(ref, sem):
        remote(ref, ref, sem, sem, sibling).wait_recv()

    def x1(kind, i):
        step, cols = ((2, low_x), (2, high_x), (1, high_x), (3, low_x), (0, None), (0, None))[kind]
        source = p16_x.at[i, rows(x, step, 64), cols] if kind < 4 else c1_x.at[kind - 4, i]
        return message(0, 0, kind, i, source)

    def y1(kind, i):
        step, cols = ((2, low_y), (2, high_y), (1, high_y), (3, low_y), (0, None), (0, None))[kind]
        source = p16_y.at[i, step, :, :, :, cols] if kind < 4 else c1_y.at[kind - 4, i]
        return message(0, 1, kind, i, source)

    def mine(step):
        return pl.ds(pl.multiple_of(x * 64 + lax.rem(hi + step, 4) * 16, 16), 16)

    def x2(kind, i):
        step, cols = ((2, low_x), (2, high_x), (1, high_x), (3, low_x), (0, None), (0, None))[kind]
        source = p16_x.at[i, mine(step), cols] if kind < 4 else c2_x.at[kind - 4, i]
        return message(1, 0, kind, i, source)

    def y2(kind, i):
        step, cols = ((2, low_y), (2, high_y), (1, high_y), (3, low_y), (0, None), (0, None))[kind]
        source = p16_y.at[i, 0, :, lax.rem(hi + step, 4), :, cols] if kind < 4 else c2_y.at[kind - 4, i]
        return message(1, 1, kind, i, source)

    def line_message(i):
        d = lax.rem(4 - roles[i], 4)
        return remote(t16_x.at[i], line.at[d], send_sem.at[2, 0, 0], last_recv.at[0], {"y": blocks[i]})

    def plane_message(i, e):
        d = lax.rem(4 - roles[i], 4)
        to = lax.rem(x + e, 4)
        n = 1 if e else 0
        return remote(
            t16_y.at[i, to], plane.at[d, (4 - e) % 4], send_sem.at[2, 1, n], last_recv.at[1 + n],
            {"y": blocks[i], "x": to},
        )

    def x_half(i, half):
        def step(j, carry):
            j = half * (HX // TILE) + j
            if i == 0:
                get_w(j).wait()
            cols = pl.ds(pl.multiple_of(j * TILE, TILE), TILE)
            part = jnp.dot(h[i], w_v[:, cols], preferred_element_type=F32)
            p32_x[i, :, cols] = part
            p16_x[i, :, cols] = part.astype(BF16)
            return carry

        lax.fori_loop(0, HX // TILE, step, 0)

    def y_quarters(i, count):
        def step(j, carry):
            r = lax.rem(5 - j, 4) if count == 3 else 2
            at = lax.rem(y + r, 4)
            if i == 0:
                get_w(WX // TILE + at).wait()
            cols = pl.ds(pl.multiple_of(WX + at * QY, QY), QY)
            part = jnp.dot(h[i], w_v[:, cols], preferred_element_type=F32).reshape(4, 4, 16, QY)
            p32_y[i, r] = part
            p16_y[i, r] = part.astype(BF16)
            return carry

        lax.fori_loop(0, count, step, 0)

    def first_product():
        with scope("first_product"):
            y_quarters(0, 1)
            x_half(0, 0)
            with scope("barrier"):
                pl.semaphore_wait(barrier, len(partners))
            gathers[1].start()
            gathers[0].start()
            for kind in (0, 1):
                y1(kind, 0).start()
            for kind in (0, 3):
                x1(kind, 0).start()
            x_half(0, 1)
            for kind in (1, 2):
                x1(kind, 0).start()
            y_quarters(0, 3)
            for kind in (2, 3):
                y1(kind, 0).start()

    def x_product(i):
        with scope(f"x_product{i}"):
            x_half(i, 0)
            x_half(i, 1)
            for kind in (0, 1):
                x1(kind, i).start()

    def y_product(i):
        with scope(f"y_product{i}"):
            y_quarters(i, 1)
            for kind in (0, 1):
                y1(kind, i).start()
            y_quarters(i, 3)

    def x_direct(i):
        for kind in (2, 3):
            x1(kind, i).start()

    def y_direct(i):
        for kind in (2, 3):
            y1(kind, i).start()

    def x_relay(i):
        with scope(f"x_relay{i}"):
            for s, step in ((0, 1), (1, 3)):
                arrived(a1_x.at[s, i], a1_recv.at[0, s, i])
                own = p32_x[i, rows(x, step, 64), s * HX : (s + 1) * HX]
                c1_x[s, i] = (own + a1_x[s, i].astype(F32)).astype(BF16)
                x1(4 + s, i).start()

    def y_relay(i):
        with scope(f"y_relay{i}"):
            for s, r in ((0, 1), (1, 3)):
                arrived(a1_y.at[s, i], a1_recv.at[1, s, i])
                own = p32_y[i, r, :, :, :, s * HY : (s + 1) * HY]
                c1_y[s, i] = (own + a1_y[s, i].astype(F32)).astype(BF16)
                y1(4 + s, i).start()

    halves = ((2, 1), (0, 3))

    def x_finish(i):
        with scope(f"x_finish{i}"):
            arrived(bc1_x.at[i], bc1_recv.at[0, i])
            own = rows(x, 0, 64)
            for s, (a, b) in enumerate(halves):
                cols = pl.ds(s * HX, HX)
                total = p32_x[i, own, cols] + bc1_x[i, a].astype(F32) + bc1_x[i, b].astype(F32)
                p32_x[i, own, cols] = total
                p16_x[i, own, cols] = total.astype(BF16)
            for kind in (0, 1, 2, 3):
                x2(kind, i).start()

    def y_finish(i):
        with scope(f"y_finish{i}"):
            arrived(bc1_y.at[i], bc1_recv.at[1, i])
            for s, (a, b) in enumerate(halves):
                cols = pl.ds(s * HY, HY)
                total = p32_y[i, 0, :, :, :, cols] + bc1_y[i, a].astype(F32) + bc1_y[i, b].astype(F32)
                p32_y[i, 0, :, :, :, cols] = total
                p16_y[i, 0, :, :, :, cols] = total.astype(BF16)
            for kind in (0, 1, 2, 3):
                y2(kind, i).start()

    def x_relay2(i):
        with scope(f"x_second{i}"):
            for s, step in ((0, 1), (1, 3)):
                arrived(a2_x.at[s, i], a2_recv.at[0, s, i])
                own = p32_x[i, mine(step), s * HX : (s + 1) * HX]
                c2_x[s, i] = (own + a2_x[s, i].astype(F32)).astype(BF16)
                x2(4 + s, i).start()

    def y_relay2(i):
        with scope(f"y_second{i}"):
            for s, step in ((0, 1), (1, 3)):
                arrived(a2_y.at[s, i], a2_recv.at[1, s, i])
                own = p32_y[i, 0, :, lax.rem(hi + step, 4), :, s * HY : (s + 1) * HY]
                c2_y[s, i] = (own + a2_y[s, i].astype(F32)).astype(BF16)
                y2(4 + s, i).start()

    def x_finish2(i):
        with scope(f"x_finish_second{i}"):
            arrived(bc2_x.at[i], bc2_recv.at[0, i])
            for s, (a, b) in enumerate(halves):
                cols = pl.ds(s * HX, HX)
                total = p32_x[i, mine(0), cols] + bc2_x[i, a].astype(F32) + bc2_x[i, b].astype(F32)
                t32_x[i, :, cols] = total
                t16_x[i, :, cols] = total.astype(LAST_X)

            @pl.when(roles[i] != 0)
            def _():
                line_message(i).start()

    def y_finish2(i):
        with scope(f"y_finish_second{i}"):
            arrived(bc2_y.at[i], bc2_recv.at[1, i])
            for s, (a, b) in enumerate(halves):
                cols = pl.ds(s * HY, HY)
                total = p32_y[i, 0, :, hi, :, cols] + bc2_y[i, a].astype(F32) + bc2_y[i, b].astype(F32)
                t32_y[i, :, :, cols] = total
                t16_y[i, :, :, cols] = total.astype(LAST_Y)
            for e in (2, 1, 3):
                plane_message(i, e).start()

            @pl.when(roles[i] != 0)
            def _():
                plane_message(i, 0).start()

    def folded(value):
        total = value[:, :128]
        for j in range(1, value.shape[1] // 128):
            total = total + value[:, j * 128 : (j + 1) * 128]
        return total

    def close(total, cols, squares):
        total = total + res_ref[:, cols].astype(F32)
        summed[:, cols] = total
        out_ref[0, :, cols] = total.astype(BF16)
        return squares + folded(total * total)

    def x_close(squares):
        with scope("x_close"):
            arrived(line.at[pl.ds(1, 3)], last_recv.at[0])
            total = t32_x[own_slot]
            for d in (1, 2, 3):
                total = total + line[d].astype(F32)
            return close(total, pl.ds(0, WX), squares)

    def y_close(squares):
        with scope("y_close"):
            arrived(plane.at[pl.ds(1, 3), 0], last_recv.at[1])
            arrived(plane.at[:, pl.ds(1, 3)], last_recv.at[2])
            for d in range(4):
                total = plane[d, 0].astype(F32) if d else t32_y[own_slot, x]
                for e in (1, 2, 3):
                    total = total + plane[d, e].astype(F32)
                squares = close(total, pl.ds(pl.multiple_of(WX + lax.rem(y + d, 4) * QY, QY), QY), squares)
            return squares

    own_slot = 2 * lax.rem(y // 2 + lo, 2) + lax.rem(y + core, 2)
    first_product()
    y_relay(0)
    with scope("gather0"):
        gathers[0].wait_recv()
    y_product(1)
    y_direct(1)
    x_relay(0)
    x_product(1)
    x_direct(1)
    y_finish(0)
    x_finish(0)
    y_relay(1)
    with scope("gather1"):
        gathers[1].wait_recv()
    gathers[2].start()
    y_product(2)
    y_direct(2)
    x_relay(1)
    y_relay2(0)
    with scope("gather2"):
        gathers[2].wait_recv()
    x_product(3)
    x_direct(3)
    x_relay2(0)
    y_finish(1)
    x_finish(1)
    y_relay(2)
    y_product(3)
    y_direct(3)
    y_relay2(1)
    x_relay(3)
    x_product(2)
    x_direct(2)
    x_relay2(1)
    y_finish(2)
    x_finish(3)
    y_relay(3)
    x_finish2(0)
    y_relay2(2)
    y_finish2(1)
    x_relay(2)
    x_finish2(1)
    x_relay2(3)
    y_finish(3)
    x_finish(2)
    y_relay2(3)
    y_finish2(0)
    y_finish2(2)
    x_relay2(2)
    x_finish2(3)
    y_finish2(3)
    x_finish2(2)
    for copy in get_rest:
        copy.wait()
    total = y_close(x_close(jnp.zeros((16, 128), F32)))

    sq_own[...] = total
    exchange = [
        remote(sq_own, sq_in.at[i], n_sem.at[0], n_sem.at[1], who)
        for i, who in enumerate((sibling, across, diagonal))
    ]
    for copy in exchange:
        copy.start()
    with scope("drain"):
        arrived(h.at[pl.ds(0, 3)], ag_send)
        for colour, (bc1, c1, bc2, c2) in enumerate(((bc1_x, c1_x, bc2_x, c2_x), (bc1_y, c1_y, bc2_y, c2_y))):
            for stage, bc, c in ((0, bc1, c1), (1, bc2, c2)):
                arrived(bc, send_sem.at[stage, colour, 0])
                arrived(c, send_sem.at[stage, colour, 1])
        arrived(line.at[pl.ds(1, 3)], send_sem.at[2, 0, 0])
        arrived(plane.at[pl.ds(1, 3), 0], send_sem.at[2, 1, 0])
        arrived(plane.at[:, pl.ds(1, 3)], send_sem.at[2, 1, 1])

    with scope("exchange"):
        arrived(sq_in, n_sem.at[1])
    for i in range(3):
        total = total + sq_in[i]
    with scope("norm"):
        scale = lax.rsqrt(jnp.sum(total, axis=1, keepdims=True) / D + 1e-05)
        for j in range(N // 128):
            cols = pl.ds(j * 128, 128)
            out_ref[1, :, cols] = (summed[:, cols] * scale * gain_ref[j : j + 1, :].astype(F32)).astype(BF16)
    arrived(sq_in, n_sem.at[0])


def body(gate_in, up_in, down_weight, residual, norm_gain):
    dma = pltpu.SemaphoreType.DMA
    vm = pltpu.VMEM
    scratch = [vm((K, 256), BF16), vm((K, 256), BF16), vm((16, N), BF16), vm((N // 128, 128), BF16), vm((KP, N), BF16), vm((4, 256, KP), BF16)]
    scratch += [vm((4, 256, WX), F32), vm((4, 256, WX), BF16)]
    scratch += [vm((4, 4, 4, 4, 16, QY), F32), vm((4, 4, 4, 4, 16, QY), BF16)]
    for rows, cols in (((64,), HX), ((4, 4, 16), HY), ((16,), HX), ((4, 16), HY)):
        scratch += [vm((2, 4, *rows, cols), BF16), vm((4, 4, *rows, cols), BF16), vm((2, 4, *rows, cols), BF16)]
    scratch += [vm((4, 16, WX), F32), vm((4, 16, WX), LAST_X), vm((4, 4, 16, QY), F32), vm((4, 4, 16, QY), LAST_Y)]
    scratch += [vm((4, 16, WX), LAST_X), vm((4, 4, 16, QY), LAST_Y)]
    scratch += [vm((16, N), F32), vm((16, 128), F32), vm((3, 16, 128), F32)]
    scratch += [dma((4,)), dma((N // TILE,)), dma, dma((3,)), dma((3, 2, 2))]
    scratch += [dma((2, 2, 4)), dma((2, 4)), dma((2, 2, 4)), dma((2, 4)), dma((3,)), dma((2,))]
    anywhere = pl.BlockSpec(memory_space=pltpu.HBM)
    vmem = pl.BlockSpec(memory_space=pltpu.VMEM)
    operands = (gate_in.T, up_in.T, down_weight, residual, norm_gain.reshape(N // 128, 128))
    operands = (pltpu.with_memory_space_constraint(a, pltpu.HBM) for a in operands)
    both = pl.pallas_call(
        kernel,
        out_shape=jax.ShapeDtypeStruct((2, 16, N), BF16),
        in_specs=[anywhere] * 5,
        out_specs=vmem,
        scratch_shapes=scratch,
        compiler_params=pltpu.CompilerParams(
            collective_id=0, has_side_effects=True, vmem_limit_bytes=VMEM_LIMIT
        ),
    )(*operands)
    return both[0], both[1]


def solution(mesh):
    split = Mesh(mesh.devices.reshape(4, 4, 4, 2, 2), ("y", "x", "h", "l", "c"))
    tp, col = ("y", "x", "h"), ("l", "c")
    return jax.shard_map(
        body,
        mesh=split,
        in_specs=(P(col, tp), P(col, tp), P(tp, col), P(tp, col), P(col)),
        out_specs=(P(tp, col), P(tp, col)),
        check_vma=False,
    )
```

```python
import functools

import jax
import jax.numpy as jnp
from jax import lax
from jax.experimental import pallas as pl
from jax.experimental.pallas import tpu as pltpu
from jax.sharding import Mesh
from jax.sharding import PartitionSpec as P

F32 = jnp.float32
BF16 = jnp.bfloat16
D = 16384
N = 4096
K = 832
KP = 896
TILE = 512
VMEM_LIMIT = 50 * 1024 * 1024
WX = 2048
WY = N - WX
HX, QY = WX // 2, WY // 4
HY = QY // 2
LAST_X = BF16
LAST_Y = BF16


def kernel(
    gate_hbm, up_hbm, w_hbm, res_hbm, gain_hbm, out_ref,
    gate_v, up_v, res_ref, gain_ref, w_v, h,
    p32_x, p16_x, p32_y, p16_y,
    a1_x, bc1_x, c1_x, a1_y, bc1_y, c1_y,
    a2_x, bc2_x, c2_x, a2_y, bc2_y, c2_y,
    t32_x, t16_x, t32_y, t16_y,
    line, plane,
    summed, sq_own, sq_in,
    in_sem, w_sem, ag_send, ag_recv, send_sem, a1_recv, bc1_recv, a2_recv, bc2_recv, last_recv, n_sem,
):
    x, y, hi, lo, core = (lax.axis_index(a) for a in ("x", "y", "h", "l", "c"))
    scope = jax.named_scope

    def ring(axis, index, step):
        return {axis: lax.rem(index + step, 4)}

    get_gate = pltpu.make_async_copy(gate_hbm, gate_v, in_sem.at[0])
    get_up = pltpu.make_async_copy(up_hbm, up_v, in_sem.at[1])
    get_gate.start()
    get_up.start()

    def get_w(j):
        cols = pl.ds(pl.multiple_of(j * TILE, TILE), TILE)
        return pltpu.make_async_copy(w_hbm.at[:, cols], w_v.at[pl.ds(0, K), cols], w_sem.at[j])

    sibling = {"c": 1 - core}
    across = {"l": 1 - lo}
    diagonal = {"l": 1 - lo, "c": 1 - core}
    partners = [sibling, across, diagonal]
    partners += [ring("h", hi, 1), ring("h", hi, 3)]
    partners += [ring("y", y, d) | ring("x", x, e) for d in range(4) for e in range(4) if d + e]

    barrier = pltpu.get_barrier_semaphore()
    for who in partners:
        pl.semaphore_signal(barrier, inc=1, device_id=who, device_id_type=pl.DeviceIdType.MESH)

    y_tile = WX // TILE
    for j in (y_tile + lax.rem(y + 2, 4), *range(HX // TILE)):
        get_w(j).start()
    w_v[K:, :] = jnp.zeros((KP - K, N), BF16)
    with scope("get_in"):
        get_gate.wait()
        get_up.wait()
    for j in (*range(HX // TILE, y_tile), *(y_tile + lax.rem(y + r, 4) for r in (1, 0, 3))):
        get_w(j).start()
    get_rest = [
        pltpu.make_async_copy(res_hbm, res_ref, in_sem.at[2]),
        pltpu.make_async_copy(gain_hbm, gain_ref, in_sem.at[3]),
    ]
    for copy in get_rest:
        copy.start()

    for k in range(KP // 128):
        depth = min(128, K - k * 128)
        g = gate_v[k * 128 : k * 128 + depth, :].astype(F32)
        u = up_v[k * 128 : k * 128 + depth, :].astype(F32)
        act = g / (1.0 + jnp.exp(-g)) * u
        if depth < 128:
            act = jnp.concatenate([act, jnp.zeros((128 - depth, 256), F32)], axis=0)
        h[0, :, k * 128 : (k + 1) * 128] = act.T.astype(BF16)

    def remote(src, dst, send, recv, who):
        return pltpu.make_async_remote_copy(
            src_ref=src, dst_ref=dst, send_sem=send, recv_sem=recv,
            device_id=who, device_id_type=pl.DeviceIdType.MESH,
        )

    gathers = [
        remote(h.at[0], h.at[1], ag_send, ag_recv.at[0], sibling),
        remote(h.at[0], h.at[2], ag_send, ag_recv.at[1], across),
        remote(h.at[2], h.at[3], ag_send, ag_recv.at[2], sibling),
    ]
    blocks = (2 * lo + core, 2 * lo + 1 - core, 2 * (1 - lo) + core, 2 * (1 - lo) + 1 - core)
    roles = [lax.rem(b + 4 - y, 4) for b in blocks]

    def rows(index, step, size):
        return pl.ds(pl.multiple_of(lax.rem(index + step, 4) * size, size), size)

    low_x, high_x = pl.ds(0, HX), pl.ds(HX, HX)
    low_y, high_y = pl.ds(0, HY), pl.ds(HY, HY)
    x_ways, y_ways, h_ways = (
        (ring(a, index, 1), ring(a, index, 3)) for a, index in (("x", x), ("y", y), ("h", hi))
    )

    def message(stage, colour, kind, i, source):
        a, bc, ways = buffers[stage][colour]
        a_recv, bc_recv = ((a1_recv, bc1_recv), (a2_recv, bc2_recv))[stage]
        if kind < 2:
            target, recv = a.at[kind, i], a_recv.at[colour, kind, i]
        else:
            target, recv = bc.at[i, kind - 2], bc_recv.at[colour, i]
        return remote(source, target, send_sem.at[stage, colour, kind // 4], recv, ways[kind % 2])

    buffers = (((a1_x, bc1_x, x_ways), (a1_y, bc1_y, y_ways)), ((a2_x, bc2_x, h_ways), (a2_y, bc2_y, h_ways)))

    def arrived(ref, sem):
        remote(ref, ref, sem, sem, sibling).wait_recv()

    def x1(kind, i):
        step, cols = ((2, low_x), (2, high_x), (1, high_x), (3, low_x), (0, None), (0, None))[kind]
        source = p16_x.at[i, rows(x, step, 64), cols] if kind < 4 else c1_x.at[kind - 4, i]
        return message(0, 0, kind, i, source)

    def y1(kind, i):
        step, cols = ((2, low_y), (2, high_y), (1, high_y), (3, low_y), (0, None), (0, None))[kind]
        source = p16_y.at[i, step, :, :, :, cols] if kind < 4 else c1_y.at[kind - 4, i]
        return message(0, 1, kind, i, source)

    def mine(step):
        return pl.ds(pl.multiple_of(x * 64 + lax.rem(hi + step, 4) * 16, 16), 16)

    def x2(kind, i):
        step, cols = ((2, low_x), (2, high_x), (1, high_x), (3, low_x), (0, None), (0, None))[kind]
        source = p16_x.at[i, mine(step), cols] if kind < 4 else c2_x.at[kind - 4, i]
        return message(1, 0, kind, i, source)

    def y2(kind, i):
        step, cols = ((2, low_y), (2, high_y), (1, high_y), (3, low_y), (0, None), (0, None))[kind]
        source = p16_y.at[i, 0, :, lax.rem(hi + step, 4), :, cols] if kind < 4 else c2_y.at[kind - 4, i]
        return message(1, 1, kind, i, source)

    def line_message(i):
        d = lax.rem(4 - roles[i], 4)
        return remote(t16_x.at[i], line.at[d], send_sem.at[2, 0, 0], last_recv.at[0], {"y": blocks[i]})

    def plane_message(i, e):
        d = lax.rem(4 - roles[i], 4)
        to = lax.rem(x + e, 4)
        n = 1 if e else 0
        return remote(
            t16_y.at[i, to], plane.at[d, (4 - e) % 4], send_sem.at[2, 1, n], last_recv.at[1 + n],
            {"y": blocks[i], "x": to},
        )

    def x_half(i, half):
        def step(j, carry):
            j = half * (HX // TILE) + j
            if i == 0:
                get_w(j).wait()
            cols = pl.ds(pl.multiple_of(j * TILE, TILE), TILE)
            part = jnp.dot(h[i], w_v[:, cols], preferred_element_type=F32)
            p32_x[i, :, cols] = part
            p16_x[i, :, cols] = part.astype(BF16)
            return carry

        lax.fori_loop(0, HX // TILE, step, 0, unroll=True)

    def y_quarters(i, count):
        def step(j, carry):
            r = lax.rem(5 - j, 4) if count == 3 else 2
            at = lax.rem(y + r, 4)
            if i == 0:
                get_w(WX // TILE + at).wait()
            cols = pl.ds(pl.multiple_of(WX + at * QY, QY), QY)
            part = jnp.dot(h[i], w_v[:, cols], preferred_element_type=F32).reshape(4, 4, 16, QY)
            p32_y[i, r] = part
            p16_y[i, r] = part.astype(BF16)
            return carry

        lax.fori_loop(0, count, step, 0, unroll=True)

    def first_product():
        with scope("first_product"):
            y_quarters(0, 1)
            x_half(0, 0)
            with scope("barrier"):
                pl.semaphore_wait(barrier, len(partners))
            gathers[1].start()
            gathers[0].start()
            for kind in (0, 1):
                y1(kind, 0).start()
            for kind in (0, 3):
                x1(kind, 0).start()
            x_half(0, 1)
            for kind in (1, 2):
                x1(kind, 0).start()
            y_quarters(0, 3)
            for kind in (2, 3):
                y1(kind, 0).start()

    def x_product(i):
        with scope(f"x_product{i}"):
            x_half(i, 0)
            x_half(i, 1)
            for kind in (0, 1):
                x1(kind, i).start()

    def y_product(i):
        with scope(f"y_product{i}"):
            y_quarters(i, 1)
            for kind in (0, 1):
                y1(kind, i).start()
            y_quarters(i, 3)

    def x_direct(i):
        for kind in (2, 3):
            x1(kind, i).start()

    def y_direct(i):
        for kind in (2, 3):
            y1(kind, i).start()

    def x_relay(i):
        with scope(f"x_relay{i}"):
            for s, step in ((0, 1), (1, 3)):
                arrived(a1_x.at[s, i], a1_recv.at[0, s, i])
                own = p32_x[i, rows(x, step, 64), s * HX : (s + 1) * HX]
                c1_x[s, i] = (own + a1_x[s, i].astype(F32)).astype(BF16)
                x1(4 + s, i).start()

    def y_relay(i):
        with scope(f"y_relay{i}"):
            for s, r in ((0, 1), (1, 3)):
                arrived(a1_y.at[s, i], a1_recv.at[1, s, i])
                own = p32_y[i, r, :, :, :, s * HY : (s + 1) * HY]
                c1_y[s, i] = (own + a1_y[s, i].astype(F32)).astype(BF16)
                y1(4 + s, i).start()

    halves = ((2, 1), (0, 3))

    def x_finish(i):
        with scope(f"x_finish{i}"):
            arrived(bc1_x.at[i], bc1_recv.at[0, i])
            own = rows(x, 0, 64)
            for s, (a, b) in enumerate(halves):
                cols = pl.ds(s * HX, HX)
                total = p32_x[i, own, cols] + bc1_x[i, a].astype(F32) + bc1_x[i, b].astype(F32)
                p32_x[i, own, cols] = total
                p16_x[i, own, cols] = total.astype(BF16)
            for kind in (0, 1, 2, 3):
                x2(kind, i).start()

    def y_finish(i):
        with scope(f"y_finish{i}"):
            arrived(bc1_y.at[i], bc1_recv.at[1, i])
            for s, (a, b) in enumerate(halves):
                cols = pl.ds(s * HY, HY)
                total = p32_y[i, 0, :, :, :, cols] + bc1_y[i, a].astype(F32) + bc1_y[i, b].astype(F32)
                p32_y[i, 0, :, :, :, cols] = total
                p16_y[i, 0, :, :, :, cols] = total.astype(BF16)
            for kind in (0, 1, 2, 3):
                y2(kind, i).start()

    def x_relay2(i):
        with scope(f"x_second{i}"):
            for s, step in ((0, 1), (1, 3)):
                arrived(a2_x.at[s, i], a2_recv.at[0, s, i])
                own = p32_x[i, mine(step), s * HX : (s + 1) * HX]
                c2_x[s, i] = (own + a2_x[s, i].astype(F32)).astype(BF16)
                x2(4 + s, i).start()

    def y_relay2(i):
        with scope(f"y_second{i}"):
            for s, step in ((0, 1), (1, 3)):
                arrived(a2_y.at[s, i], a2_recv.at[1, s, i])
                own = p32_y[i, 0, :, lax.rem(hi + step, 4), :, s * HY : (s + 1) * HY]
                c2_y[s, i] = (own + a2_y[s, i].astype(F32)).astype(BF16)
                y2(4 + s, i).start()

    def x_finish2(i):
        with scope(f"x_finish_second{i}"):
            arrived(bc2_x.at[i], bc2_recv.at[0, i])
            for s, (a, b) in enumerate(halves):
                cols = pl.ds(s * HX, HX)
                total = p32_x[i, mine(0), cols] + bc2_x[i, a].astype(F32) + bc2_x[i, b].astype(F32)
                t32_x[i, :, cols] = total
                t16_x[i, :, cols] = total.astype(LAST_X)

            @pl.when(roles[i] != 0)
            def _():
                line_message(i).start()

    def y_finish2(i):
        with scope(f"y_finish_second{i}"):
            arrived(bc2_y.at[i], bc2_recv.at[1, i])
            for s, (a, b) in enumerate(halves):
                cols = pl.ds(s * HY, HY)
                total = p32_y[i, 0, :, hi, :, cols] + bc2_y[i, a].astype(F32) + bc2_y[i, b].astype(F32)
                t32_y[i, :, :, cols] = total
                t16_y[i, :, :, cols] = total.astype(LAST_Y)
            for e in (2, 1, 3):
                plane_message(i, e).start()

            @pl.when(roles[i] != 0)
            def _():
                plane_message(i, 0).start()

    def folded(value):
        total = value[:, :128]
        for j in range(1, value.shape[1] // 128):
            total = total + value[:, j * 128 : (j + 1) * 128]
        return total

    def close(total, cols, squares):
        total = total + res_ref[:, cols].astype(F32)
        summed[:, cols] = total
        out_ref[0, :, cols] = total.astype(BF16)
        return squares + folded(total * total)

    def x_close(squares):
        with scope("x_close"):
            arrived(line.at[pl.ds(1, 3)], last_recv.at[0])
            total = t32_x[own_slot]
            for d in (1, 2, 3):
                total = total + line[d].astype(F32)
            return close(total, pl.ds(0, WX), squares)

    def y_close(squares):
        with scope("y_close"):
            arrived(plane.at[pl.ds(1, 3), 0], last_recv.at[1])
            arrived(plane.at[:, pl.ds(1, 3)], last_recv.at[2])
            for d in range(4):
                total = plane[d, 0].astype(F32) if d else t32_y[own_slot, x]
                for e in (1, 2, 3):
                    total = total + plane[d, e].astype(F32)
                squares = close(total, pl.ds(pl.multiple_of(WX + lax.rem(y + d, 4) * QY, QY), QY), squares)
            return squares

    own_slot = 2 * lax.rem(y // 2 + lo, 2) + lax.rem(y + core, 2)
    first_product()
    with scope("gather0"):
        gathers[0].wait_recv()
    x_product(1)
    y_relay(0)
    x_relay(0)
    y_product(1)
    x_direct(1)
    y_direct(1)
    y_finish(0)
    x_relay(1)
    x_finish(0)
    with scope("gather1"):
        gathers[1].wait_recv()
    gathers[2].start()
    y_relay(1)
    x_product(2)
    y_relay2(0)
    y_product(2)
    y_direct(2)
    x_relay2(0)
    y_finish(1)
    x_direct(2)
    with scope("gather2"):
        gathers[2].wait_recv()
    x_product(3)
    x_finish(1)
    y_relay(2)
    y_product(3)
    y_relay2(1)
    x_relay(2)
    y_direct(3)
    x_relay2(1)
    y_finish(2)
    y_relay(3)
    x_direct(3)
    x_finish(2)
    y_finish2(0)
    x_relay(3)
    y_relay2(2)
    x_finish2(0)
    x_relay2(2)
    y_finish(3)
    y_finish2(2)
    x_finish(3)
    x_finish2(2)
    y_relay2(3)
    y_finish2(1)
    x_relay2(3)
    y_finish2(3)
    x_finish2(1)
    x_finish2(3)
    for copy in get_rest:
        copy.wait()
    total = y_close(x_close(jnp.zeros((16, 128), F32)))

    sq_own[...] = total
    exchange = [
        remote(sq_own, sq_in.at[i], n_sem.at[0], n_sem.at[1], who)
        for i, who in enumerate((sibling, across, diagonal))
    ]
    for copy in exchange:
        copy.start()
    with scope("drain"):
        arrived(h.at[pl.ds(0, 3)], ag_send)
        for colour, (bc1, c1, bc2, c2) in enumerate(((bc1_x, c1_x, bc2_x, c2_x), (bc1_y, c1_y, bc2_y, c2_y))):
            for stage, bc, c in ((0, bc1, c1), (1, bc2, c2)):
                arrived(bc, send_sem.at[stage, colour, 0])
                arrived(c, send_sem.at[stage, colour, 1])
        arrived(line.at[pl.ds(1, 3)], send_sem.at[2, 0, 0])
        arrived(plane.at[pl.ds(1, 3), 0], send_sem.at[2, 1, 0])
        arrived(plane.at[:, pl.ds(1, 3)], send_sem.at[2, 1, 1])

    with scope("exchange"):
        arrived(sq_in, n_sem.at[1])
    for i in range(3):
        total = total + sq_in[i]
    with scope("norm"):
        scale = lax.rsqrt(jnp.sum(total, axis=1, keepdims=True) / D + 1e-05)
        for j in range(N // 128):
            cols = pl.ds(j * 128, 128)
            out_ref[1, :, cols] = (summed[:, cols] * scale * gain_ref[j : j + 1, :].astype(F32)).astype(BF16)
    arrived(sq_in, n_sem.at[0])


def body(gate_in, up_in, down_weight, residual, norm_gain):
    dma = pltpu.SemaphoreType.DMA
    vm = pltpu.VMEM
    scratch = [vm((K, 256), BF16), vm((K, 256), BF16), vm((16, N), BF16), vm((N // 128, 128), BF16), vm((KP, N), BF16), vm((4, 256, KP), BF16)]
    scratch += [vm((4, 256, WX), F32), vm((4, 256, WX), BF16)]
    scratch += [vm((4, 4, 4, 4, 16, QY), F32), vm((4, 4, 4, 4, 16, QY), BF16)]
    for rows, cols in (((64,), HX), ((4, 4, 16), HY), ((16,), HX), ((4, 16), HY)):
        scratch += [vm((2, 4, *rows, cols), BF16), vm((4, 4, *rows, cols), BF16), vm((2, 4, *rows, cols), BF16)]
    scratch += [vm((4, 16, WX), F32), vm((4, 16, WX), LAST_X), vm((4, 4, 16, QY), F32), vm((4, 4, 16, QY), LAST_Y)]
    scratch += [vm((4, 16, WX), LAST_X), vm((4, 4, 16, QY), LAST_Y)]
    scratch += [vm((16, N), F32), vm((16, 128), F32), vm((3, 16, 128), F32)]
    scratch += [dma((4,)), dma((N // TILE,)), dma, dma((3,)), dma((3, 2, 2))]
    scratch += [dma((2, 2, 4)), dma((2, 4)), dma((2, 2, 4)), dma((2, 4)), dma((3,)), dma((2,))]
    anywhere = pl.BlockSpec(memory_space=pltpu.HBM)
    vmem = pl.BlockSpec(memory_space=pltpu.VMEM)
    operands = (gate_in.T, up_in.T, down_weight, residual, norm_gain.reshape(N // 128, 128))
    operands = (pltpu.with_memory_space_constraint(a, pltpu.HBM) for a in operands)
    both = pl.pallas_call(
        kernel,
        out_shape=jax.ShapeDtypeStruct((2, 16, N), BF16),
        in_specs=[anywhere] * 5,
        out_specs=vmem,
        scratch_shapes=scratch,
        compiler_params=pltpu.CompilerParams(
            collective_id=0, has_side_effects=True, vmem_limit_bytes=VMEM_LIMIT
        ),
    )(*operands)
    return both[0], both[1]


def solution(mesh):
    split = Mesh(mesh.devices.reshape(4, 4, 4, 2, 2), ("y", "x", "h", "l", "c"))
    tp, col = ("y", "x", "h"), ("l", "c")
    return jax.shard_map(
        body,
        mesh=split,
        in_specs=(P(col, tp), P(col, tp), P(tp, col), P(tp, col), P(col)),
        out_specs=(P(tp, col), P(tp, col)),
        check_vma=False,
    )
```

```python
import functools

import jax
import jax.numpy as jnp
from jax import lax
from jax.experimental import pallas as pl
from jax.experimental.pallas import tpu as pltpu
from jax.sharding import Mesh
from jax.sharding import PartitionSpec as P

F32 = jnp.float32
BF16 = jnp.bfloat16
D = 16384
N = 4096
K = 832
KP = 896
TILE = 512
VMEM_LIMIT = 50 * 1024 * 1024
WX = 2048
WY = N - WX
HX, QY = WX // 2, WY // 4
HY = QY // 2
LAST_X = BF16
LAST_Y = BF16


def kernel(
    gate_hbm, up_hbm, w_hbm, res_hbm, gain_hbm, out_ref,
    gate_v, up_v, res_ref, gain_ref, w_v, h,
    p32_x, p16_x, p32_y, p16_y,
    a1_x, bc1_x, c1_x, a1_y, bc1_y, c1_y,
    a2_x, bc2_x, c2_x, a2_y, bc2_y, c2_y,
    t32_x, t16_x, t32_y, t16_y,
    line, plane,
    summed, sq_own, sq_in,
    in_sem, w_sem, ag_send, ag_recv, send_sem, a1_recv, bc1_recv, a2_recv, bc2_recv, last_recv, n_sem,
):
    x, y, hi, lo, core = (lax.axis_index(a) for a in ("x", "y", "h", "l", "c"))
    scope = jax.named_scope

    def ring(axis, index, step):
        return {axis: lax.rem(index + step, 4)}

    get_gate = pltpu.make_async_copy(gate_hbm, gate_v, in_sem.at[0])
    get_up = pltpu.make_async_copy(up_hbm, up_v, in_sem.at[1])
    get_gate.start()
    get_up.start()

    def get_w(j):
        cols = pl.ds(pl.multiple_of(j * TILE, TILE), TILE)
        return pltpu.make_async_copy(w_hbm.at[:, cols], w_v.at[pl.ds(0, K), cols], w_sem.at[j])

    sibling = {"c": 1 - core}
    across = {"l": 1 - lo}
    diagonal = {"l": 1 - lo, "c": 1 - core}
    partners = [sibling, across, diagonal]
    partners += [ring("h", hi, 1), ring("h", hi, 3)]
    partners += [ring("y", y, d) | ring("x", x, e) for d in range(4) for e in range(4) if d + e]

    barrier = pltpu.get_barrier_semaphore()
    for who in partners:
        pl.semaphore_signal(barrier, inc=1, device_id=who, device_id_type=pl.DeviceIdType.MESH)

    y_tile = WX // TILE
    for j in (y_tile + lax.rem(y + 2, 4), *range(HX // TILE)):
        get_w(j).start()
    w_v[K:, :] = jnp.zeros((KP - K, N), BF16)
    with scope("get_in"):
        get_gate.wait()
        get_up.wait()
    for j in (*range(HX // TILE, y_tile), *(y_tile + lax.rem(y + r, 4) for r in (1, 0, 3))):
        get_w(j).start()
    get_rest = [
        pltpu.make_async_copy(res_hbm, res_ref, in_sem.at[2]),
        pltpu.make_async_copy(gain_hbm, gain_ref, in_sem.at[3]),
    ]
    for copy in get_rest:
        copy.start()

    for k in range(KP // 128):
        depth = min(128, K - k * 128)
        g = gate_v[k * 128 : k * 128 + depth, :].astype(F32)
        u = up_v[k * 128 : k * 128 + depth, :].astype(F32)
        act = g / (1.0 + jnp.exp(-g)) * u
        if depth < 128:
            act = jnp.concatenate([act, jnp.zeros((128 - depth, 256), F32)], axis=0)
        h[0, :, k * 128 : (k + 1) * 128] = act.T.astype(BF16)

    def remote(src, dst, send, recv, who):
        return pltpu.make_async_remote_copy(
            src_ref=src, dst_ref=dst, send_sem=send, recv_sem=recv,
            device_id=who, device_id_type=pl.DeviceIdType.MESH,
        )

    gathers = [
        remote(h.at[0], h.at[1], ag_send, ag_recv.at[0], sibling),
        remote(h.at[0], h.at[2], ag_send, ag_recv.at[1], across),
        remote(h.at[2], h.at[3], ag_send, ag_recv.at[2], sibling),
    ]
    blocks = (2 * lo + core, 2 * lo + 1 - core, 2 * (1 - lo) + core, 2 * (1 - lo) + 1 - core)
    roles = [lax.rem(b + 4 - y, 4) for b in blocks]

    def rows(index, step, size):
        return pl.ds(pl.multiple_of(lax.rem(index + step, 4) * size, size), size)

    low_x, high_x = pl.ds(0, HX), pl.ds(HX, HX)
    low_y, high_y = pl.ds(0, HY), pl.ds(HY, HY)
    x_ways, y_ways, h_ways = (
        (ring(a, index, 1), ring(a, index, 3)) for a, index in (("x", x), ("y", y), ("h", hi))
    )

    def message(stage, colour, kind, i, source):
        a, bc, ways = buffers[stage][colour]
        a_recv, bc_recv = ((a1_recv, bc1_recv), (a2_recv, bc2_recv))[stage]
        if kind < 2:
            target, recv = a.at[kind, i], a_recv.at[colour, kind, i]
        else:
            target, recv = bc.at[i, kind - 2], bc_recv.at[colour, i]
        return remote(source, target, send_sem.at[stage, colour, kind // 4], recv, ways[kind % 2])

    buffers = (((a1_x, bc1_x, x_ways), (a1_y, bc1_y, y_ways)), ((a2_x, bc2_x, h_ways), (a2_y, bc2_y, h_ways)))

    def arrived(ref, sem):
        remote(ref, ref, sem, sem, sibling).wait_recv()

    def x1(kind, i):
        step, cols = ((2, low_x), (2, high_x), (1, high_x), (3, low_x), (0, None), (0, None))[kind]
        source = p16_x.at[i, rows(x, step, 64), cols] if kind < 4 else c1_x.at[kind - 4, i]
        return message(0, 0, kind, i, source)

    def y1(kind, i):
        step, cols = ((2, low_y), (2, high_y), (1, high_y), (3, low_y), (0, None), (0, None))[kind]
        source = p16_y.at[i, step, :, :, :, cols] if kind < 4 else c1_y.at[kind - 4, i]
        return message(0, 1, kind, i, source)

    def mine(step):
        return pl.ds(pl.multiple_of(x * 64 + lax.rem(hi + step, 4) * 16, 16), 16)

    def x2(kind, i):
        step, cols = ((2, low_x), (2, high_x), (1, high_x), (3, low_x), (0, None), (0, None))[kind]
        source = p16_x.at[i, mine(step), cols] if kind < 4 else c2_x.at[kind - 4, i]
        return message(1, 0, kind, i, source)

    def y2(kind, i):
        step, cols = ((2, low_y), (2, high_y), (1, high_y), (3, low_y), (0, None), (0, None))[kind]
        source = p16_y.at[i, 0, :, lax.rem(hi + step, 4), :, cols] if kind < 4 else c2_y.at[kind - 4, i]
        return message(1, 1, kind, i, source)

    def line_message(i):
        d = lax.rem(4 - roles[i], 4)
        return remote(t16_x.at[i], line.at[d], send_sem.at[2, 0, 0], last_recv.at[0], {"y": blocks[i]})

    def plane_message(i, e):
        d = lax.rem(4 - roles[i], 4)
        to = lax.rem(x + e, 4)
        n = 1 if e else 0
        return remote(
            t16_y.at[i, to], plane.at[d, (4 - e) % 4], send_sem.at[2, 1, n], last_recv.at[1 + n],
            {"y": blocks[i], "x": to},
        )

    def x_half(i, half):
        def step(j, carry):
            j = half * (HX // TILE) + j
            if i == 0:
                get_w(j).wait()
            cols = pl.ds(pl.multiple_of(j * TILE, TILE), TILE)
            part = jnp.dot(h[i], w_v[:, cols], preferred_element_type=F32)
            p32_x[i, :, cols] = part
            p16_x[i, :, cols] = part.astype(BF16)
            return carry

        lax.fori_loop(0, HX // TILE, step, 0, unroll=True)

    def y_quarters(i, count):
        def step(j, carry):
            r = lax.rem(5 - j, 4) if count == 3 else 2
            at = lax.rem(y + r, 4)
            if i == 0:
                get_w(WX // TILE + at).wait()
            cols = pl.ds(pl.multiple_of(WX + at * QY, QY), QY)
            part = jnp.dot(h[i], w_v[:, cols], preferred_element_type=F32).reshape(4, 4, 16, QY)
            p32_y[i, r] = part
            p16_y[i, r] = part.astype(BF16)
            return carry

        lax.fori_loop(0, count, step, 0, unroll=True)

    def first_product():
        with scope("first_product"):
            y_quarters(0, 1)
            x_half(0, 0)
            x_half(0, 1)
            with scope("barrier"):
                pl.semaphore_wait(barrier, len(partners))
            gathers[1].start()
            gathers[0].start()
            for kind in (0, 1):
                y1(kind, 0).start()
            for kind in (0, 1, 2, 3):
                x1(kind, 0).start()
            y_quarters(0, 3)
            for kind in (2, 3):
                y1(kind, 0).start()

    def x_product(i):
        with scope(f"x_product{i}"):
            x_half(i, 0)
            x_half(i, 1)
            for kind in (0, 1):
                x1(kind, i).start()

    def y_product(i):
        with scope(f"y_product{i}"):
            y_quarters(i, 1)
            for kind in (0, 1):
                y1(kind, i).start()
            y_quarters(i, 3)

    def x_direct(i):
        for kind in (2, 3):
            x1(kind, i).start()

    def y_direct(i):
        for kind in (2, 3):
            y1(kind, i).start()

    def x_relay(i):
        with scope(f"x_relay{i}"):
            for s, step in ((0, 1), (1, 3)):
                arrived(a1_x.at[s, i], a1_recv.at[0, s, i])
                own = p32_x[i, rows(x, step, 64), s * HX : (s + 1) * HX]
                c1_x[s, i] = (own + a1_x[s, i].astype(F32)).astype(BF16)
                x1(4 + s, i).start()

    def y_relay(i):
        with scope(f"y_relay{i}"):
            for s, r in ((0, 1), (1, 3)):
                arrived(a1_y.at[s, i], a1_recv.at[1, s, i])
                own = p32_y[i, r, :, :, :, s * HY : (s + 1) * HY]
                c1_y[s, i] = (own + a1_y[s, i].astype(F32)).astype(BF16)
                y1(4 + s, i).start()

    halves = ((2, 1), (0, 3))

    def x_finish(i):
        with scope(f"x_finish{i}"):
            arrived(bc1_x.at[i], bc1_recv.at[0, i])
            own = rows(x, 0, 64)
            for s, (a, b) in enumerate(halves):
                cols = pl.ds(s * HX, HX)
                total = p32_x[i, own, cols] + bc1_x[i, a].astype(F32) + bc1_x[i, b].astype(F32)
                p32_x[i, own, cols] = total
                p16_x[i, own, cols] = total.astype(BF16)
            for kind in (0, 1, 2, 3):
                x2(kind, i).start()

    def y_finish(i):
        with scope(f"y_finish{i}"):
            arrived(bc1_y.at[i], bc1_recv.at[1, i])
            for s, (a, b) in enumerate(halves):
                cols = pl.ds(s * HY, HY)
                total = p32_y[i, 0, :, :, :, cols] + bc1_y[i, a].astype(F32) + bc1_y[i, b].astype(F32)
                p32_y[i, 0, :, :, :, cols] = total
                p16_y[i, 0, :, :, :, cols] = total.astype(BF16)
            for kind in (0, 1, 2, 3):
                y2(kind, i).start()

    def x_relay2(i):
        with scope(f"x_second{i}"):
            for s, step in ((0, 1), (1, 3)):
                arrived(a2_x.at[s, i], a2_recv.at[0, s, i])
                own = p32_x[i, mine(step), s * HX : (s + 1) * HX]
                c2_x[s, i] = (own + a2_x[s, i].astype(F32)).astype(BF16)
                x2(4 + s, i).start()

    def y_relay2(i):
        with scope(f"y_second{i}"):
            for s, step in ((0, 1), (1, 3)):
                arrived(a2_y.at[s, i], a2_recv.at[1, s, i])
                own = p32_y[i, 0, :, lax.rem(hi + step, 4), :, s * HY : (s + 1) * HY]
                c2_y[s, i] = (own + a2_y[s, i].astype(F32)).astype(BF16)
                y2(4 + s, i).start()

    def x_finish2(i):
        with scope(f"x_finish_second{i}"):
            arrived(bc2_x.at[i], bc2_recv.at[0, i])
            for s, (a, b) in enumerate(halves):
                cols = pl.ds(s * HX, HX)
                total = p32_x[i, mine(0), cols] + bc2_x[i, a].astype(F32) + bc2_x[i, b].astype(F32)
                t32_x[i, :, cols] = total
                t16_x[i, :, cols] = total.astype(LAST_X)

            @pl.when(roles[i] != 0)
            def _():
                line_message(i).start()

    def y_finish2(i):
        with scope(f"y_finish_second{i}"):
            arrived(bc2_y.at[i], bc2_recv.at[1, i])
            for s, (a, b) in enumerate(halves):
                cols = pl.ds(s * HY, HY)
                total = p32_y[i, 0, :, hi, :, cols] + bc2_y[i, a].astype(F32) + bc2_y[i, b].astype(F32)
                t32_y[i, :, :, cols] = total
                t16_y[i, :, :, cols] = total.astype(LAST_Y)
            for e in (2, 1, 3):
                plane_message(i, e).start()

            @pl.when(roles[i] != 0)
            def _():
                plane_message(i, 0).start()

    def folded(value):
        total = value[:, :128]
        for j in range(1, value.shape[1] // 128):
            total = total + value[:, j * 128 : (j + 1) * 128]
        return total

    def close(total, cols, squares):
        total = total + res_ref[:, cols].astype(F32)
        summed[:, cols] = total
        out_ref[0, :, cols] = total.astype(BF16)
        return squares + folded(total * total)

    def x_close(squares):
        with scope("x_close"):
            arrived(line.at[pl.ds(1, 3)], last_recv.at[0])
            total = t32_x[own_slot]
            for d in (1, 2, 3):
                total = total + line[d].astype(F32)
            return close(total, pl.ds(0, WX), squares)

    def y_close(squares):
        with scope("y_close"):
            arrived(plane.at[pl.ds(1, 3), 0], last_recv.at[1])
            arrived(plane.at[:, pl.ds(1, 3)], last_recv.at[2])
            for d in range(4):
                total = plane[d, 0].astype(F32) if d else t32_y[own_slot, x]
                for e in (1, 2, 3):
                    total = total + plane[d, e].astype(F32)
                squares = close(total, pl.ds(pl.multiple_of(WX + lax.rem(y + d, 4) * QY, QY), QY), squares)
            return squares

    own_slot = 2 * lax.rem(y // 2 + lo, 2) + lax.rem(y + core, 2)
    first_product()
    with scope("gather0"):
        gathers[0].wait_recv()
    x_product(1)
    y_relay(0)
    x_relay(0)
    y_product(1)
    x_direct(1)
    y_direct(1)
    y_finish(0)
    x_relay(1)
    x_finish(0)
    with scope("gather1"):
        gathers[1].wait_recv()
    gathers[2].start()
    y_relay(1)
    x_product(2)
    y_relay2(0)
    y_product(2)
    y_direct(2)
    x_relay2(0)
    y_finish(1)
    x_direct(2)
    with scope("gather2"):
        gathers[2].wait_recv()
    x_product(3)
    x_finish(1)
    y_relay(2)
    y_product(3)
    y_relay2(1)
    x_relay(2)
    y_direct(3)
    x_relay2(1)
    y_finish(2)
    y_relay(3)
    x_direct(3)
    x_finish(2)
    y_finish2(0)
    x_relay(3)
    y_relay2(2)
    x_finish2(0)
    x_relay2(2)
    y_finish(3)
    y_finish2(2)
    x_finish(3)
    x_finish2(2)
    y_relay2(3)
    y_finish2(1)
    x_relay2(3)
    y_finish2(3)
    x_finish2(1)
    x_finish2(3)
    for copy in get_rest:
        copy.wait()
    total = y_close(x_close(jnp.zeros((16, 128), F32)))

    sq_own[...] = total
    exchange = [
        remote(sq_own, sq_in.at[i], n_sem.at[0], n_sem.at[1], who)
        for i, who in enumerate((sibling, across, diagonal))
    ]
    for copy in exchange:
        copy.start()
    with scope("drain"):
        arrived(h.at[pl.ds(0, 3)], ag_send)
        for colour, (bc1, c1, bc2, c2) in enumerate(((bc1_x, c1_x, bc2_x, c2_x), (bc1_y, c1_y, bc2_y, c2_y))):
            for stage, bc, c in ((0, bc1, c1), (1, bc2, c2)):
                arrived(bc, send_sem.at[stage, colour, 0])
                arrived(c, send_sem.at[stage, colour, 1])
        arrived(line.at[pl.ds(1, 3)], send_sem.at[2, 0, 0])
        arrived(plane.at[pl.ds(1, 3), 0], send_sem.at[2, 1, 0])
        arrived(plane.at[:, pl.ds(1, 3)], send_sem.at[2, 1, 1])

    with scope("exchange"):
        arrived(sq_in, n_sem.at[1])
    for i in range(3):
        total = total + sq_in[i]
    with scope("norm"):
        scale = lax.rsqrt(jnp.sum(total, axis=1, keepdims=True) / D + 1e-05)
        for j in range(N // 128):
            cols = pl.ds(j * 128, 128)
            out_ref[1, :, cols] = (summed[:, cols] * scale * gain_ref[j : j + 1, :].astype(F32)).astype(BF16)
    arrived(sq_in, n_sem.at[0])


def body(gate_in, up_in, down_weight, residual, norm_gain):
    dma = pltpu.SemaphoreType.DMA
    vm = pltpu.VMEM
    scratch = [vm((K, 256), BF16), vm((K, 256), BF16), vm((16, N), BF16), vm((N // 128, 128), BF16), vm((KP, N), BF16), vm((4, 256, KP), BF16)]
    scratch += [vm((4, 256, WX), F32), vm((4, 256, WX), BF16)]
    scratch += [vm((4, 4, 4, 4, 16, QY), F32), vm((4, 4, 4, 4, 16, QY), BF16)]
    for rows, cols in (((64,), HX), ((4, 4, 16), HY), ((16,), HX), ((4, 16), HY)):
        scratch += [vm((2, 4, *rows, cols), BF16), vm((4, 4, *rows, cols), BF16), vm((2, 4, *rows, cols), BF16)]
    scratch += [vm((4, 16, WX), F32), vm((4, 16, WX), LAST_X), vm((4, 4, 16, QY), F32), vm((4, 4, 16, QY), LAST_Y)]
    scratch += [vm((4, 16, WX), LAST_X), vm((4, 4, 16, QY), LAST_Y)]
    scratch += [vm((16, N), F32), vm((16, 128), F32), vm((3, 16, 128), F32)]
    scratch += [dma((4,)), dma((N // TILE,)), dma, dma((3,)), dma((3, 2, 2))]
    scratch += [dma((2, 2, 4)), dma((2, 4)), dma((2, 2, 4)), dma((2, 4)), dma((3,)), dma((2,))]
    anywhere = pl.BlockSpec(memory_space=pltpu.HBM)
    vmem = pl.BlockSpec(memory_space=pltpu.VMEM)
    operands = (gate_in.T, up_in.T, down_weight, residual, norm_gain.reshape(N // 128, 128))
    operands = (pltpu.with_memory_space_constraint(a, pltpu.HBM) for a in operands)
    both = pl.pallas_call(
        kernel,
        out_shape=jax.ShapeDtypeStruct((2, 16, N), BF16),
        in_specs=[anywhere] * 5,
        out_specs=vmem,
        scratch_shapes=scratch,
        compiler_params=pltpu.CompilerParams(
            collective_id=0, has_side_effects=True, vmem_limit_bytes=VMEM_LIMIT
        ),
    )(*operands)
    return both[0], both[1]


def solution(mesh):
    split = Mesh(mesh.devices.reshape(4, 4, 4, 2, 2), ("y", "x", "h", "l", "c"))
    tp, col = ("y", "x", "h"), ("l", "c")
    return jax.shard_map(
        body,
        mesh=split,
        in_specs=(P(col, tp), P(col, tp), P(tp, col), P(tp, col), P(col)),
        out_specs=(P(tp, col), P(tp, col)),
        check_vma=False,
    )
```
